128 devices in a mesh: rep: 1, dp: 128 (over x, y, z, core).
Axes of the slice: x: 4, y: 4, z: 4, core: 2. Of those that a mesh axis runs over, the one named last changes fastest.
Arguments:
- x: bfloat16 [128, 1024, 640], P(('rep', 'dp'))
- dy: bfloat16 [128, 1024, 640], P(('rep', 'dp'))
- wq: bfloat16 [1, 640, 640], replicated
- wk: bfloat16 [1, 640, 128], replicated
- wv: bfloat16 [1, 640, 128], replicated
- wo: bfloat16 [1, 640, 640], replicated
- w_gate: bfloat16 [1, 640, 3456], replicated
- w_up: bfloat16 [1, 640, 3456], replicated
- w_down: bfloat16 [1, 3456, 640], replicated
- m_wq: float32 [1, 640, 640], replicated
- m_wk: float32 [1, 640, 128], replicated
- m_wv: float32 [1, 640, 128], replicated
- m_wo: float32 [1, 640, 640], replicated
- m_w_gate: float32 [1, 640, 3456], replicated
- m_w_up: float32 [1, 640, 3456], replicated
- m_w_down: float32 [1, 3456, 640], replicated
- v_wq: float32 [1, 640, 640], replicated
- v_wk: float32 [1, 640, 128], replicated
- v_wv: float32 [1, 640, 128], replicated
- v_wo: float32 [1, 640, 640], replicated
- v_w_gate: float32 [1, 640, 3456], replicated
- v_w_up: float32 [1, 640, 3456], replicated
- v_w_down: float32 [1, 3456, 640], replicated
Outputs:
- output 1: bfloat16 [1, 640, 640], P('rep')
- output 2: bfloat16 [1, 640, 128], P('rep')
- output 3: bfloat16 [1, 640, 128], P('rep')
- output 4: bfloat16 [1, 640, 640], P('rep')
- output 5: bfloat16 [1, 640, 3456], P('rep')
- output 6: bfloat16 [1, 640, 3456], P('rep')
- output 7: bfloat16 [1, 3456, 640], P('rep')
- output 8: float32 [1, 640, 640], P('rep')
- output 9: float32 [1, 640, 128], P('rep')
- output 10: float32 [1, 640, 128], P('rep')
- output 11: float32 [1, 640, 640], P('rep')
- output 12: float32 [1, 640, 3456], P('rep')
- output 13: float32 [1, 640, 3456], P('rep')
- output 14: float32 [1, 3456, 640], P('rep')
- output 15: float32 [1, 640, 640], P('rep')
- output 16: float32 [1, 640, 128], P('rep')
- output 17: float32 [1, 640, 128], P('rep')
- output 18: float32 [1, 640, 640], P('rep')
- output 19: float32 [1, 640, 3456], P('rep')
- output 20: float32 [1, 640, 3456], P('rep')
- output 21: float32 [1, 3456, 640], P('rep')
All inputs are finite; a program needn't handle non-finite values.
Results may differ from the reference program's by a relative error of at most 0.024.
Values are sent between devices in bfloat16 or wider.
A program may use at most 1.5 GiB of HBM per device.

```python
import jax
import jax.numpy as jnp
from jax import lax

SEQUENCES = 128
TOKENS = 1024
D = 640
HEADS = 5
KV_HEADS = 1
HEAD = 128
FF = 3456
LAYERS = 1
THETA = 10000
NAMES = ("wq", "wk", "wv", "wo", "w_gate", "w_up", "w_down")
SHAPES = {
    "wq": (LAYERS, D, HEADS * HEAD),
    "wk": (LAYERS, D, KV_HEADS * HEAD),
    "wv": (LAYERS, D, KV_HEADS * HEAD),
    "wo": (LAYERS, HEADS * HEAD, D),
    "w_gate": (LAYERS, D, FF),
    "w_up": (LAYERS, D, FF),
    "w_down": (LAYERS, FF, D),
}


def bump(key, n, height):
    away = (jnp.arange(n, dtype=jnp.int32) - jax.random.randint(key, (), 0, n, jnp.int32)) % n
    return jnp.where(away < n // 8, height, 1.0)


def together(key, own, strength):
    shared = jax.random.normal(key, own.shape[1:], jnp.float32)
    return (own + strength * shared) * lax.rsqrt(1 + strength * strength)


def setup_inputs(seed: int = 0, part: int = 0) -> dict:
    kx, kdy, ka, kb, kz, kf, kh, kl, *keys = jax.random.split(jax.random.key(seed), 8 + 3 * len(NAMES))
    kx, kdy, ka, kb = (jax.random.fold_in(k, part) for k in (kx, kdy, ka, kb))
    kw, km, kv = (keys[i::3] for i in range(3))
    shape = (SEQUENCES, TOKENS, D)
    much_x, much_dy = jax.random.uniform(kz, (2,), jnp.float32, 0.0, 1.0)
    loud = 2.0 ** jax.random.uniform(jax.random.fold_in(kz, 1), (), jnp.float32, -1.0, 2.0)
    layers = 2.0 ** jax.random.uniform(kl, (LAYERS, 1, 1), jnp.float32, -1.0, 1.0)
    times = {"wq": 1.0, "wk": 1.0, "wv": 2.0, "wo": layers, "w_gate": 1.0, "w_up": bump(kh, FF, 4.0), "w_down": layers}
    x = together(ka, jax.random.normal(kx, shape, jnp.float32), much_x) * bump(kf, D, 4.0)
    dy = together(kb, jax.random.normal(kdy, shape, jnp.float32), much_dy)
    drawn = {"x": x.astype(jnp.bfloat16), "dy": (loud * dy * (SEQUENCES * TOKENS) ** -0.5).astype(jnp.bfloat16)}
    for key, name in zip(kw, NAMES, strict=True):
        drawn[name] = (jax.random.normal(key, SHAPES[name], jnp.float32) * SHAPES[name][1] ** -0.5 * times[name]).astype(jnp.bfloat16)
    for key, name in zip(km, NAMES, strict=True):
        drawn[f"m_{name}"] = 0.1 * jax.random.normal(key, SHAPES[name], jnp.float32)
    for key, name in zip(kv, NAMES, strict=True):
        drawn[f"v_{name}"] = jax.random.uniform(key, SHAPES[name], jnp.float32, 0.02, 0.06)
    return drawn


def matmul(a, w):
    return jnp.dot(a, w, preferred_element_type=jnp.float32).astype(jnp.bfloat16)


def normed(h):
    wide = h.astype(jnp.float32)
    scale = lax.rsqrt(jnp.mean(wide**2, -1, keepdims=True) + 1e-6)
    return (wide * scale).astype(jnp.bfloat16)


def turned(t, theta):
    half = t.shape[-1] // 2
    angle = jnp.arange(t.shape[0], dtype=jnp.float32)[:, None] * theta ** (-jnp.arange(half, dtype=jnp.float32) / half)
    cos, sin = jnp.cos(angle)[:, None], jnp.sin(angle)[:, None]
    a, b = t[..., :half].astype(jnp.float32), t[..., half:].astype(jnp.float32)
    return jnp.concatenate([a * cos - b * sin, b * cos + a * sin], -1).astype(jnp.bfloat16)


def seen_by(q, k, v):
    tokens, kv = q.shape[0], k.shape[1]
    q = q.reshape(tokens, kv, -1, q.shape[-1])
    scores = jnp.einsum("tgsd,ugd->gstu", q.astype(jnp.float32), k.astype(jnp.float32)) * q.shape[-1] ** -0.5
    place = jnp.arange(tokens)
    weights = jax.nn.softmax(jnp.where(place[:, None] >= place, scores, -jnp.inf), -1).astype(jnp.bfloat16)
    return jnp.einsum("gstu,ugd->tgsd", weights.astype(jnp.float32), v.astype(jnp.float32)).astype(jnp.bfloat16).reshape(tokens, -1)


def layer(h, w):
    a = normed(h)
    q, k = (turned(matmul(a, w[name]).reshape(h.shape[0], -1, HEAD), THETA) for name in ("wq", "wk"))
    h = h + matmul(seen_by(q, k, matmul(a, w["wv"]).reshape(h.shape[0], -1, HEAD)), w["wo"])
    b = normed(h)
    gate = jnp.dot(b, w["w_gate"], preferred_element_type=jnp.float32)
    up = jnp.dot(b, w["w_up"], preferred_element_type=jnp.float32)
    return h + matmul((jax.nn.silu(gate) * up).astype(jnp.bfloat16), w["w_down"])


def adamw(w, m, v, g):
    m = 0.9 * m + 0.1 * g
    v = 0.95 * v + 0.05 * g * g
    step = m * lax.rsqrt(v + 1e-8) + 0.1 * w
    return (w - 0.02 * step).astype(jnp.bfloat16), m, v


def clipped(gradients, sum_of_squares, count):
    factor = jnp.minimum(1.0, 0.5 * lax.rsqrt(sum_of_squares / count + 1e-30))
    return [g * factor for g in gradients]


def stack(weights, h):
    return lax.scan(lambda h, w: (layer(h, w), None), h, weights)[0]


def reference(x, dy, wq, wk, wv, wo, w_gate, w_up, w_down, m_wq, m_wk, m_wv, m_wo, m_w_gate, m_w_up, m_w_down, v_wq, v_wk, v_wv, v_wo, v_w_gate, v_w_up, v_w_down):
    weights = dict(zip(NAMES, (wq, wk, wv, wo, w_gate, w_up, w_down), strict=True))

    def take(so_far, sequence):
        h, by_y = sequence
        _, back = jax.vjp(stack, weights, h)
        by_weights, by_h = back(by_y)
        return jax.tree.map(lambda total, term: total + term.astype(jnp.float32), so_far, by_weights), by_h

    none_yet = {name: jnp.zeros(w.shape, jnp.float32) for name, w in weights.items()}
    by_weights, by_x = lax.scan(take, none_yet, (x, dy))
    gradients = [by_weights[name].astype(jnp.bfloat16).astype(jnp.float32) for name in NAMES]
    gradients = clipped(gradients, sum(jnp.sum(g * g) for g in gradients), sum(g.size for g in gradients))
    first = (m_wq, m_wk, m_wv, m_wo, m_w_gate, m_w_up, m_w_down)
    second = (v_wq, v_wk, v_wv, v_wo, v_w_gate, v_w_up, v_w_down)
    new = [adamw(weights[name].astype(jnp.float32), m, v, g) for name, m, v, g in zip(NAMES, first, second, gradients, strict=True)]
    return tuple(one[which] for which in range(3) for one in new)
```

```python
import functools

import jax
import jax.numpy as jnp
import numpy as np
from jax import lax
from jax.experimental import pallas as pl
from jax.experimental.pallas import tpu as pltpu
from jax.sharding import PartitionSpec as P

BF16, F32 = jnp.bfloat16, jnp.float32
LANES = 128
TOKENS, D, HEADS, FF = 1024, 640, 5, 3456
HEAD, HALF = LANES, LANES // 2
THETA = 10000
HIDDEN = -1e30
SCALE = HEAD**-0.5
LOG2E = 1.4426950408889634
VMEM = 56 * 2**20
STRIP = 256
EIGHTH, DOWN = 80, 48
WAVES, BLOCK = 9, 384
WAVE, ATTN = 240, 400
MLP = WAVES * WAVE
ROWS = MLP + ATTN
STRIDES = (32, 8, 2)
ORDERS = ((0, 1, 2), (1, 2, 0), (2, 0, 1))
COLOURS = range(3)
TILE = 16
PER_CORE, PIECES = 12, 24


def _dot(a, b, ca, cb):
    return lax.dot_general(a, b, (((ca,), (cb,)), ((), ())), preferred_element_type=F32)


def _nn(a, b):
    return _dot(a, b, 1, 0)


def _nt(a, b):
    return _dot(a, b, 1, 1)


def _scale(wide):
    return lax.rsqrt(jnp.mean(wide * wide, -1, keepdims=True) + 1e-6)


def _span(n, size):
    return slice(n * size, n * size + size)


def _lanes(n):
    return _span(n, LANES)


def _turning(turns_ref, rows):
    table = turns_ref[rows, :]
    other = pltpu.roll(table, HALF, 1)
    first = lax.broadcasted_iota(jnp.int32, table.shape, 1) < HALF
    return jnp.where(first, table, other), jnp.where(first, -other, table)


def _hide(s, first_key, first_query):
    key = lax.broadcasted_iota(jnp.int32, s.shape, 0) + first_key
    query = lax.broadcasted_iota(jnp.int32, s.shape, 1) + first_query
    return jnp.where(query >= key, s, HIDDEN)


def _front(x_ref, turns_ref, wq_ref, wk_ref, wv_ref, wo_ref, *rest):
    outs, held, (vt_s, sem) = rest[:8], rest[8:16], rest[16:]
    q_s, k_s, v_s, o_s, h_s, b_s, bt_s, lse_s = held
    copies = []
    wkv = jnp.concatenate([wk_ref[...], wv_ref[...]], axis=1)
    vt_s[HEAD:, :] = jnp.ones((vt_s.shape[0] - HEAD, TOKENS), BF16)
    for i in range(TOKENS // STRIP):
        rows = _span(i, STRIP)
        keys = rows.stop
        x = x_ref[rows, :].astype(F32)
        a = (x * _scale(x)).astype(BF16)
        cos, sin = _turning(turns_ref, rows)

        def turned(t):
            t = t.astype(BF16).astype(F32)
            return (t * cos + pltpu.roll(t, HALF, 1) * sin).astype(BF16)

        q = _nn(a, wq_ref[...])
        for g in range(HEADS):
            q_s[g, rows, :] = turned(q[:, _lanes(g)])
        kv = _nn(a, wkv)
        k_s[rows, :] = turned(kv[:, :HEAD])
        v = kv[:, HEAD:].astype(BF16)
        v_s[rows, :] = v
        vt_s[:HEAD, rows] = v.T
        for g in range(HEADS):
            s = _nt(k_s[:keys, :], q_s[g, rows, :])
            own = _hide(s[i * STRIP :, :], 0, 0)
            s = own if i == 0 else jnp.concatenate([s[: i * STRIP, :], own], axis=0)
            top = jnp.max(s, axis=0, keepdims=True)
            p = jnp.exp2((s - top) * (SCALE * LOG2E)).astype(BF16)
            mix = _nn(vt_s[:, :keys], p)
            total = mix[HEAD : HEAD + 1, :]
            o_s[rows, _lanes(g)] = (mix[:HEAD, :] * (1 / total)).T.astype(BF16)
            lse_s[g, :, rows] = top * (SCALE * LOG2E) + jnp.log2(total)
        h = (x + _nn(o_s[rows, :], wo_ref[...]).astype(BF16).astype(F32)).astype(BF16)
        h_s[rows, :] = h
        h = h.astype(F32)
        b = (h * _scale(h)).astype(BF16)
        b_s[rows, :] = b
        bt_s[:, rows] = b.T
        for src, dst in zip(held, outs, strict=True):
            if src is q_s:
                src, dst = src.at[:, rows, :], dst.at[:, rows, :]
            elif src is bt_s:
                src, dst = src.at[:, rows], dst.at[:, rows]
            elif src is lse_s:
                src, dst = src.at[:, :, rows], dst.at[:, :, rows]
            else:
                src, dst = src.at[rows, :], dst.at[rows, :]
            copies.append(pltpu.make_async_copy(src, dst, sem.at[len(copies)]))
            copies[-1].start()
    for copy in copies:
        copy.wait()


def _params(**more):
    return pltpu.CompilerParams(vmem_limit_bytes=VMEM, **more)


def _turns():
    angle = np.arange(TOKENS)[:, None] * float(THETA) ** (-np.arange(HALF) / HALF)
    return jnp.asarray(np.concatenate([np.cos(angle), np.sin(angle)], 1), F32)


ANYWHERE = pl.BlockSpec(memory_space=pl.ANY)
IN_VMEM = pl.BlockSpec(memory_space=pltpu.VMEM)


def front(x, turns, wq, wk, wv, wo):
    shapes = [((HEADS, TOKENS, HEAD), BF16), ((TOKENS, HEAD), BF16), ((TOKENS, HEAD), BF16), ((TOKENS, D), BF16), ((TOKENS, D), BF16),
              ((TOKENS, D), BF16), ((D, TOKENS), BF16), ((HEADS, 1, TOKENS), F32)]
    return pl.pallas_call(
        _front,
        in_specs=[IN_VMEM] * 6,
        out_specs=[ANYWHERE] * 8,
        out_shape=[jax.ShapeDtypeStruct(*one) for one in shapes],
        scratch_shapes=[pltpu.VMEM(*one) for one in shapes] + [pltpu.VMEM((HEAD + 8, TOKENS), BF16), pltpu.SemaphoreType.DMA((32,))],
        compiler_params=_params(),
        cost_estimate=pl.CostEstimate(flops=5 * 10**9, transcendentals=4 * 10**6, bytes_accessed=15 * 10**6),
        name="front",
    )(x, turns, wq, wk, wv, wo)


def _mlp(b_ref, bt_ref, dy_ref, wg_ref, wu_ref, wd_ref, g_ref, db_ref, acc):
    f = pl.program_id(0)
    wgu = jnp.concatenate([wg_ref[...], wu_ref[...]], axis=1)
    gu = _nn(b_ref[...], wgu)
    gate, up = gu[:, :BLOCK], gu[:, BLOCK:]
    dact = _nt(dy_ref[...], wd_ref[...]).astype(BF16).astype(F32)
    s = 0.5 * jnp.tanh(0.5 * gate) + 0.5
    silu = gate * s
    act = (silu * up).astype(BF16)
    dgu = jnp.concatenate([(dact * up * (s + silu * (1 - s))).astype(BF16), (dact * silu).astype(BF16)], axis=1)
    dw = _nn(bt_ref[...], dgu).astype(BF16)
    dwd = _dot(act, dy_ref[...], 0, 0).astype(BF16)
    for r in range(8):
        j = r // 4 * PER_CORE + r % 4
        for k in range(2):
            for t in range(3):
                g_ref[0, j + 4 * k, _span(t, EIGHTH), :] = dw[_span(r, EIGHTH), _lanes(3 * k + t)]
        for t in range(5):
            g_ref[0, j + 8, _span(t, DOWN), :] = dwd[_span(r, DOWN), _lanes(t)]
    more = _nt(dgu, wgu)

    @pl.when(f == 0)
    def _():
        acc[...] = more

    @pl.when(f > 0)
    def _():
        acc[...] += more

    @pl.when(f == WAVES - 1)
    def _():
        db_ref[...] = acc[...].astype(BF16)


def mlp(b, bt, dy, wg, wu, wd):
    whole = lambda *shape: pl.BlockSpec(shape, lambda f: (0, 0))
    across, down = pl.BlockSpec((D, BLOCK), lambda f: (0, f)), pl.BlockSpec((BLOCK, D), lambda f: (f, 0))
    return pl.pallas_call(
        _mlp,
        grid=(WAVES,),
        in_specs=[whole(TOKENS, D), whole(D, TOKENS), whole(TOKENS, D), across, across, down],
        out_specs=[pl.BlockSpec((1, PIECES, WAVE, LANES), lambda f: (f, 0, 0, 0)), whole(TOKENS, D)],
        out_shape=[jax.ShapeDtypeStruct((WAVES, PIECES, WAVE, LANES), BF16), jax.ShapeDtypeStruct((TOKENS, D), BF16)],
        scratch_shapes=[pltpu.VMEM((TOKENS, D), F32)],
        compiler_params=_params(dimension_semantics=("arbitrary",)),
        cost_estimate=pl.CostEstimate(flops=16 * TOKENS * D * FF, transcendentals=TOKENS * FF, bytes_accessed=40 * 2**20),
        name="mlp",
    )(b, bt, dy, wg, wu, wd)


def _back(x_ref, dy_ref, db_ref, h_ref, q_ref, k_ref, v_ref, o_ref, lse_ref, turns_ref, wo_ref, ga_ref,
          at_s, ot_s, dh_s, do_s, delta_s, kt_s, dq_s, dk_s, dv_s):
    strips = range(TOKENS // STRIP)
    kt_s[...] = k_ref[...].T
    dk_s[...] = jnp.zeros_like(dk_s)
    dv_s[...] = jnp.zeros_like(dv_s)

    def turned_back(t, rows):
        t = t.astype(BF16).astype(F32)
        cos, sin = _turning(turns_ref, rows)
        return (t * cos + pltpu.roll(t * sin, HALF, 1)).astype(BF16)

    for i in strips:
        rows = _span(i, STRIP)
        keys = rows.stop
        h, db = h_ref[rows, :].astype(F32), db_ref[rows, :].astype(F32)
        scale = _scale(h)
        by_scale = jnp.sum(db * h, -1, keepdims=True)
        dh = (db * scale - h * (by_scale * scale * scale * scale * (1 / D))).astype(BF16).astype(F32)
        dh = (dy_ref[rows, :].astype(F32) + dh).astype(BF16)
        dh_s[rows, :] = dh
        do = _nt(dh, wo_ref[...]).astype(BF16)
        o = o_ref[rows, :]
        ot_s[:, rows] = o.T
        x = x_ref[rows, :].astype(F32)
        at_s[:, rows] = (x * _scale(x)).astype(BF16).T
        for g in range(HEADS):
            do_s[g, rows, :] = do[:, _lanes(g)]
            both = do[:, _lanes(g)].astype(F32) * o[:, _lanes(g)].astype(F32)
            delta_s[g, :, rows] = jnp.sum(both.T, axis=0, keepdims=True)

        def head(g):
            q, do_g = q_ref[g, rows, :], do_s[g, rows, :]
            s = _nt(k_ref[:keys, :], q)
            own = _hide(s[i * STRIP :, :], 0, 0)
            s = own if i == 0 else jnp.concatenate([s[: i * STRIP, :], own], axis=0)
            p = jnp.exp2(s * (SCALE * LOG2E) - lse_ref[g, :, rows])
            ds = (p * (_nt(v_ref[:keys, :], do_g) - delta_s[g, :, rows])).astype(BF16)
            dv_s[:keys, :] += _nn(p.astype(BF16), do_g)
            dk_s[:keys, :] += _nn(ds, q)
            dq = (_nn(kt_s[:, :keys], ds) * SCALE).T
            dq_s[g, rows, :] = turned_back(dq, rows)

        pl.loop(0, HEADS)(head)

    every = slice(None)
    dqkv = [dq_s[g] for g in range(HEADS)] + [turned_back(dk_s[...] * SCALE, every), dv_s[...].astype(BF16)]
    dqkv = _nn(at_s[...], jnp.concatenate(dqkv, axis=1)).astype(BF16)
    dwo = _nn(ot_s[...], dh_s[...]).astype(BF16)
    for r in range(8):
        j, rows = r // 4 * PER_CORE + r % 4, _span(r, EIGHTH)
        for t in range(HEADS):
            here = _span(t, EIGHTH)
            ga_ref[j, here, :] = dqkv[rows, _lanes(t)]
            ga_ref[j + 4, here, :] = dwo[rows, _lanes(t)]
            ga_ref[j + 8, here, :] = dqkv[rows, _lanes(HEADS + t)] if t < 2 else jnp.zeros((EIGHTH, LANES), BF16)


def back(x, dy, db, h, q, k, v, o, lse, turns, wo):
    vmem = lambda *shape: pltpu.VMEM(shape, BF16)
    return pl.pallas_call(
        _back,
        in_specs=[IN_VMEM] * 11,
        out_specs=IN_VMEM,
        out_shape=jax.ShapeDtypeStruct((PIECES, ATTN, LANES), BF16),
        scratch_shapes=[vmem(D, TOKENS), vmem(D, TOKENS), vmem(TOKENS, D), vmem(HEADS, TOKENS, HEAD), pltpu.VMEM((HEADS, 1, TOKENS), F32),
                        vmem(HEAD, TOKENS), vmem(HEADS, TOKENS, HEAD), pltpu.VMEM((TOKENS, HEAD), F32), pltpu.VMEM((TOKENS, HEAD), F32)],
        compiler_params=_params(),
        cost_estimate=pl.CostEstimate(flops=8 * 10**9, transcendentals=4 * 10**6, bytes_accessed=15 * 10**6),
        name="back",
    )(x, dy, db, h, q, k, v, o, lse, turns, wo)


def _reduce(gm, ga, out_m, out_a, nrm, am, aa, rm, ra, lo_m, hi_m, hi_a, b_m, b_a, a1, s2, r2a, r2b, a2, s3, r3a, r3b, w, ns, nd, ssem, rsem, lsem):
    me = lax.axis_index("dp")
    core = lax.rem(me, 2)
    at = [lax.rem(lax.div(me, s), 4) for s in STRIDES]

    def along(d, q):
        return me + STRIDES[d] * (lax.rem(at[d] + q, 4) - at[d])

    plus, minus = [along(d, 1) for d in range(3)], [along(d, 3) for d in range(3)]
    partner = me + 1 - 2 * core
    barrier = pltpu.get_barrier_semaphore()
    for other in (*plus, *minus, partner):
        pl.semaphore_signal(barrier, inc=1, device_id={"dp": other}, device_id_type=pl.DeviceIdType.MESH)
    pl.semaphore_wait(barrier, 7)

    count, locals_ = [0], [0]
    sent = []

    def send(src, dst, other):
        n = count[0]
        count[0] += 1
        copy = pltpu.make_async_remote_copy(src_ref=src, dst_ref=dst, send_sem=ssem.at[n], recv_sem=rsem.at[n], device_id={"dp": other},
                                            device_id_type=pl.DeviceIdType.MESH)
        copy.start()
        sent.append(copy)
        return copy

    def local(src, dst):
        n = locals_[0]
        locals_[0] += 1
        copy = pltpu.make_async_copy(src, dst, lsem.at[n])
        copy.start()
        return copy

    def loop(n, body):
        pl.loop(0, n)(body)

    def wide(ref, *where):
        return ref[where].astype(F32)

    firsts = [[4 * k + lax.rem(at[ORDERS[k][0]] + q, 4) for q in range(4)] for k in COLOURS]

    halves = {}
    for q in (2, 1, 3, 0):
        for k in COLOURS:
            j = firsts[k][q]
            theirs, mine = (1 - core) * PER_CORE + j, core * PER_CORE + j
            halves[q, k] = [send(gm.at[:, theirs], rm.at[j], partner), send(ga.at[theirs], ra.at[j], partner)], [
                local(gm.at[:, mine], am.at[j]), local(ga.at[mine], aa.at[j])]

    def have(q, k):
        for copy in halves[q, k][0]:
            copy.wait_recv()
        for copy in halves[q, k][1]:
            copy.wait()

    def wave(j, i, *more):
        total = wide(am, j, i) + wide(rm, j, i)
        for ref, *where in more:
            total += wide(ref, *where)
        am[j, i] = total.astype(BF16)

    def attn(j, i, *more):
        here = pl.ds(i * EIGHTH, EIGHTH)
        total = wide(aa, j, here) + wide(ra, j, here)
        for ref, *where in more:
            total += wide(ref, *where, here)
        aa[j, here] = total.astype(BF16)

    step1, step2 = {}, {}
    for k in COLOURS:
        d, j = ORDERS[k][0], firsts[k][2]
        have(2, k)
        loop(WAVES, lambda i: wave(j, i))
        loop(HEADS, lambda i: attn(j, i))
        step1[k] = [send(am.at[j, :LO], lo_m.at[k], plus[d]), send(am.at[j, LO:], hi_m.at[k], minus[d]), send(aa.at[j], hi_a.at[k], minus[d])]
    for k in COLOURS:
        d, j = ORDERS[k][0], firsts[k][1]
        have(1, k)
        step1[k][0].wait_recv()
        loop(LO, lambda i: wave(j, i, (lo_m, k, i)))
        loop(WAVES - LO, lambda i: wave(j, i + LO))
        loop(HEADS, lambda i: attn(j, i))
        step2[k] = [send(am.at[j], b_m.at[k, 0], plus[d]), send(aa.at[j], b_a.at[k, 0], plus[d])]
        j = firsts[k][3]
        have(3, k)
        step1[k][1].wait_recv()
        step1[k][2].wait_recv()
        loop(LO, lambda i: wave(j, i))
        loop(WAVES - LO, lambda i: wave(j, i + LO, (hi_m, k, i)))
        loop(HEADS, lambda i: attn(j, i, (hi_a, k)))
        step2[k] += [send(am.at[j], b_m.at[k, 1], minus[d]), send(aa.at[j], b_a.at[k, 1], minus[d])]
    for k in COLOURS:
        j = firsts[k][0]
        have(0, k)
        for copy in step2[k]:
            copy.wait_recv()

        def own(i):
            a1[k, pl.ds(pl.multiple_of(i * WAVE, TILE), WAVE)] = wide(am, j, i) + wide(rm, j, i) + wide(b_m, k, 0, i) + wide(b_m, k, 1, i)

        def own_attn(i):
            here = pl.ds(i * EIGHTH, EIGHTH)
            total = wide(aa, j, here) + wide(ra, j, here) + wide(b_a, k, 0, here) + wide(b_a, k, 1, here)
            a1[k, pl.ds(pl.multiple_of(MLP + i * EIGHTH, TILE), EIGHTH)] = total

        loop(WAVES, own)
        loop(HEADS, own_attn)

    def ring(dim, size, a, s, ra_, rb, chunk, store):
        half, n = size // 2, size // chunk
        first, second = {}, {}

        def block(k, q):
            return lax.rem(at[ORDERS[k][dim]] + q, 4) * size

        def place(start, i):
            return pl.ds(pl.multiple_of(start + i * chunk, TILE), chunk)

        for k in COLOURS:
            d, o = ORDERS[k][dim], block(k, 2)

            def far(i):
                s[k, 0, place(0, i)] = a[k, place(o, i)].astype(BF16)

            loop(n, far)
            first[k] = [send(s.at[k, 0, :half], ra_.at[k, 0], plus[d]), send(s.at[k, 0, half:], ra_.at[k, 1], minus[d])]
        for k in COLOURS:
            d, p, m = ORDERS[k][dim], block(k, 1), block(k, 3)

            def relayed(i, c=None):
                s[k, 1, place(0, i)] = (a[k, place(p, i)] + wide(ra_, k, 0, place(0, i))).astype(BF16)

            def plain(i):
                s[k, 1, place(half, i)] = a[k, place(p + half, i)].astype(BF16)

            def relayed_m(i):
                s[k, 2, place(half, i)] = (a[k, place(m + half, i)] + wide(ra_, k, 1, place(0, i))).astype(BF16)

            def plain_m(i):
                s[k, 2, place(0, i)] = a[k, place(m, i)].astype(BF16)

            first[k][0].wait_recv()
            loop(n // 2, relayed)
            loop(n // 2, plain)
            second[k] = [send(s.at[k, 1], rb.at[k, 0], plus[d])]
            first[k][1].wait_recv()
            loop(n // 2, relayed_m)
            loop(n // 2, plain_m)
            second[k] += [send(s.at[k, 2], rb.at[k, 1], minus[d])]
        for k in COLOURS:
            for copy in second[k]:
                copy.wait_recv()
            own = block(k, 0)
            loop(n, lambda i: store(k, i, a[k, place(own, i)] + wide(rb, k, 0, place(0, i)) + wide(rb, k, 1, place(0, i))))

    def keep(k, i, total):
        a2[k, pl.ds(pl.multiple_of(i * 160, TILE), 160)] = total

    def finish(k, i, total):
        start = at[ORDERS[k][1]] * 640 + at[ORDERS[k][2]] * 160 + i * 80
        rounded = total.astype(BF16)
        w[firsts[k][0], pl.ds(pl.multiple_of(start, TILE), 80)] = rounded
        again = rounded.astype(F32)
        ns[2, at[2]] += jnp.sum((again * again).reshape(10, 8, 128), axis=0)

    ns[2, at[2]] = jnp.zeros((8, 128), F32)
    ring(1, 640, a1, s2, r2a, r2b, 160, keep)
    ring(2, 160, a2, s3, r3a, r3b, 80, finish)

    def squares(d, move):
        slot = lax.rem(at[d] + 3 * (move == 1), 4)
        return send(ns.at[d, slot], ns.at[d, slot],
                    minus[d] if move == 2 else plus[d])

    out_copies = []

    def finished(k, q):
        j = firsts[k][q]
        for src, dst in ((w.at[j, :MLP], out_m), (w.at[j, MLP:], out_a)):
            dst = dst.at[core * PER_CORE + j]
            out_copies.append((local(src, dst), send(src, dst, partner)))

    for dim, size in ((2, 160), (1, 640), (0, ROWS)):

        def rows(k, q, start, n):
            base = {2: at[ORDERS[k][1]] * 640, 1: 0, 0: 0}[dim]
            if dim:
                base = base + lax.rem(at[ORDERS[k][dim]] + q, 4) * size
            return w.at[firsts[k][0 if dim else q], pl.ds(pl.multiple_of(base + start, TILE), n)]

        first, second = {}, {}
        for k in COLOURS:
            d = ORDERS[k][dim]
            first[k] = [send(rows(k, 0, 0, size), rows(k, 0, 0, size), plus[d]), send(rows(k, 0, 0, size), rows(k, 0, 0, size), minus[d])]
        if dim == 0:
            for k in COLOURS:
                finished(k, 0)
        squared = [squares(dim, 0), squares(dim, 2)]
        for k in COLOURS:
            d = ORDERS[k][dim]
            first[k][0].wait_recv()
            second[k] = [send(rows(k, 3, 0, size // 2), rows(k, 3, 0, size // 2), plus[d])]
            first[k][1].wait_recv()
            second[k] += [send(rows(k, 1, size // 2, size // 2), rows(k, 1, size // 2, size // 2), minus[d])]
            if dim == 0:
                finished(k, 3)
                finished(k, 1)
        for copy in squared:
            copy.wait_recv()
        squared = squares(dim, 1)
        for k in COLOURS:
            for copy in second[k]:
                copy.wait_recv()
            if dim == 0:
                finished(k, 2)
        squared.wait_recv()
        total = ns[dim, 0] + ns[dim, 1] + ns[dim, 2] + ns[dim, 3]
        if dim:
            ns[dim - 1, at[dim - 1]] = total
        else:
            nd[core] = total
    pair = send(nd.at[core], nd.at[core], partner)
    pair.wait_recv()
    nrm[...] = nd[0] + nd[1]
    for here, there in out_copies:
        here.wait()
        there.wait_recv()
    for copy in sent:
        copy.wait_send()


def reduce_all(gm, ga):
    vmem = lambda *shape: pltpu.VMEM((*shape, LANES), BF16)
    wide = lambda *shape: pltpu.VMEM((*shape, LANES), F32)
    q2, q3 = ROWS // 4, ROWS // 16
    sizes = (
        vmem(PER_CORE, WAVES, WAVE), vmem(PER_CORE, ATTN), vmem(PER_CORE, WAVES, WAVE), vmem(PER_CORE, ATTN),
        vmem(3, LO, WAVE), vmem(3, WAVES - LO, WAVE), vmem(3, ATTN), vmem(3, 2, WAVES, WAVE), vmem(3, 2, ATTN),
        wide(3, ROWS), vmem(3, 3, q2), vmem(3, 2, q2 // 2), vmem(3, 2, q2),
        wide(3, q2), vmem(3, 3, q3), vmem(3, 2, q3 // 2), vmem(3, 2, q3),
        vmem(PER_CORE, ROWS), wide(3, 4, 8), wide(2, 8),
        pltpu.SemaphoreType.DMA((160,)), pltpu.SemaphoreType.DMA((160,)), pltpu.SemaphoreType.DMA((60,)),
    )
    return pl.pallas_call(
        _reduce,
        in_specs=[ANYWHERE] * 2,
        out_specs=[ANYWHERE] * 2 + [IN_VMEM],
        out_shape=[jax.ShapeDtypeStruct((PIECES, MLP, LANES), BF16), jax.ShapeDtypeStruct((PIECES, ATTN, LANES), BF16),
                   jax.ShapeDtypeStruct((8, LANES), F32)],
        scratch_shapes=sizes,
        compiler_params=_params(collective_id=0, has_side_effects=True),
        cost_estimate=pl.CostEstimate(flops=10**8, transcendentals=0, bytes_accessed=64 * 2**20),
        name="reduce_all",
    )(gm, ga)


def adamw(w, m, v, g):
    m = 0.9 * m + 0.1 * g
    v = 0.95 * v + 0.05 * g * g
    step = m * lax.rsqrt(v + 1e-8) + 0.1 * w
    return (w - 0.02 * step).astype(BF16), m, v


LO = 5
THIRD = WAVES // 3


def _adam(nrm_ref, gm_ref, ga_ref, *refs):
    total = jnp.sum(jnp.sum(nrm_ref[...], axis=0, keepdims=True), axis=1, keepdims=True)
    factor = jnp.minimum(1.0, 0.5 * lax.rsqrt(total / (3 * D * FF + 2 * D * (D + HEAD)) + 1e-30))
    wq, wk, wv, wo, gate, up, down = (refs[i::7] for i in range(7))

    def step(refs, where, g):
        w, m, v, new_w, new_m, new_v = refs
        new_w[where], new_m[where], new_v[where] = adamw(w[where].astype(F32), m[where], v[where], g.astype(F32) * factor)

    for n in range(THIRD):
        for t in range(3):
            here = _span(3 * n + t, EIGHTH)
            for k, refs in enumerate((gate, up)):
                step(refs, (slice(None), _lanes(3 * n + t)), gm_ref[0, k, 0, here, :])
        for t in range(5):
            here = _span(5 * n + t, DOWN)
            step(down, (n, 0, slice(None), _lanes(t)), gm_ref[0, 2, 0, here, :])

    @pl.when(pl.program_id(1) == 2)
    def _():
        for k, refs in enumerate((wq, wo)):
            for t in range(HEADS):
                step(refs, (slice(None), _lanes(t)), ga_ref[0, k, 0, _span(t, EIGHTH), :])
        for t, refs in enumerate((wk, wv)):
            step(refs, (slice(None), slice(None)), ga_ref[0, 2, 0, _span(t, EIGHTH), :])


def adam(nrm, gm, ga, *wmv):
    small = lambda width: pl.BlockSpec((EIGHTH, width), lambda r, i: (r, 0))
    across = pl.BlockSpec((EIGHTH, THIRD * BLOCK), lambda r, i: (r, i))
    specs = [small(D), small(HEAD), small(HEAD), small(D), across, across, pl.BlockSpec((THIRD, 1, DOWN, D), lambda r, i: (i, r, 0, 0))] * 3
    given = [one.reshape(WAVES, 8, DOWN, D) if one.shape[0] == FF else one for one in wmv]
    pieces = lambda g: g.reshape(2, 3, 4, -1, LANES)
    got = pl.pallas_call(
        _adam,
        grid=(8, 3),
        in_specs=[
            pl.BlockSpec((8, LANES), lambda r, i: (0, 0)),
            pl.BlockSpec((1, 3, 1, THIRD * WAVE, LANES), lambda r, i: (r // 4, 0, r % 4, i, 0)),
            pl.BlockSpec((1, 3, 1, ATTN, LANES), lambda r, i: (r // 4, 0, r % 4, 0, 0)),
            *specs,
        ],
        out_specs=specs,
        out_shape=[jax.ShapeDtypeStruct(one.shape, one.dtype) for one in given],
        compiler_params=_params(dimension_semantics=("arbitrary", "arbitrary")),
        cost_estimate=pl.CostEstimate(flops=10**8, transcendentals=8 * 10**6, bytes_accessed=168 * 10**6),
        name="adam",
    )(nrm, pieces(gm), pieces(ga), *given)
    return [one.reshape(was.shape) for one, was in zip(got, wmv, strict=True)]


def solution(mesh):
    def step(x, dy, *arrays):
        x, dy = x[0], dy[0]
        given = [one[0] for one in arrays]
        wq, wk, wv, wo, gate, up, down = given[:7]
        turns = _turns()
        q, k, v, o, h, b, bt, lse = front(x, turns, wq, wk, wv, wo)
        gm, db = mlp(b, bt, dy, gate, up, down)
        ga = back(x, dy, db, h, q, k, v, o, lse, turns, wo)
        gm, ga, nrm = reduce_all(gm, ga)
        return tuple(one[None] for one in adam(nrm, gm, ga, *given))

    states, all_of = P(("rep", "dp"), None, None), P(None, None, None)
    return jax.shard_map(
        step,
        mesh=mesh,
        in_specs=(states, states) + (all_of,) * 21,
        out_specs=(P("rep", None, None),) * 21,
        check_vma=False,
    )
```

```python
import math

import jax
import jax.numpy as jnp
import numpy as np
from jax import lax
from jax.experimental import pallas as pl
from jax.experimental.pallas import tpu as pltpu
from jax.sharding import PartitionSpec as P

BF16, F32 = jnp.bfloat16, jnp.float32
LANES = 128
TOKENS, D, HEADS, FF = 1024, 640, 5, 3456
HEAD, HALF = LANES, LANES // 2
THETA = 10000
HIDDEN = -1e30
SCALE = HEAD**-0.5
LOG2E = 1.4426950408889634
VMEM = 56 * 2**20
STRIP = 256
EIGHTH, DOWN = 80, 48
WAVES, BLOCK = 9, 384
WAVE, ATTN = 240, 400
MLP = WAVES * WAVE
ROWS = MLP + ATTN
LOW = 128
SIDE = 4
NEXT, FAR, LAST = 1, 2, 3
Q2, Q3 = ROWS // 4, ROWS // 16
STRIDES = (32, 8, 2)
ORDERS = ((0, 1, 2), (1, 2, 0), (2, 0, 1))
COLOURS = range(3)
TILE = 16
PER_CORE, PIECES = 12, 24


def _dot(a, b, ca, cb):
    return lax.dot_general(a, b, (((ca,), (cb,)), ((), ())), preferred_element_type=F32)


def _nn(a, b):
    return _dot(a, b, 1, 0)


def _nt(a, b):
    return _dot(a, b, 1, 1)


def _scale(wide):
    return lax.rsqrt(jnp.mean(wide * wide, -1, keepdims=True) + 1e-6)


def _span(n, size):
    return slice(n * size, n * size + size)


def _lanes(n):
    return _span(n, LANES)


def _turning(turns_ref, rows):
    table = turns_ref[rows, :]
    other = pltpu.roll(table, HALF, 1)
    first = lax.broadcasted_iota(jnp.int32, table.shape, 1) < HALF
    return jnp.where(first, table, other), jnp.where(first, -other, table)


def _hide(s, first_key, first_query):
    key = lax.broadcasted_iota(jnp.int32, s.shape, 0) + first_key
    query = lax.broadcasted_iota(jnp.int32, s.shape, 1) + first_query
    return jnp.where(query >= key, s, HIDDEN)


def _front(x_ref, turns_ref, wq_ref, wk_ref, wv_ref, wo_ref, *rest):
    outs, held, (vt_s, sem) = rest[:8], rest[8:16], rest[16:]
    q_s, k_s, v_s, o_s, h_s, b_s, bt_s, lse_s = held
    copies = []
    wkv = jnp.concatenate([wk_ref[...], wv_ref[...]], axis=1)
    vt_s[HEAD:, :] = jnp.ones((vt_s.shape[0] - HEAD, TOKENS), BF16)
    for i in range(TOKENS // STRIP):
        rows = _span(i, STRIP)
        keys = rows.stop
        x = x_ref[rows, :].astype(F32)
        a = (x * _scale(x)).astype(BF16)
        cos, sin = _turning(turns_ref, rows)

        def turned(t):
            t = t.astype(BF16).astype(F32)
            return (t * cos + pltpu.roll(t, HALF, 1) * sin).astype(BF16)

        q = _nn(a, wq_ref[...])
        for g in range(HEADS):
            q_s[g, rows, :] = turned(q[:, _lanes(g)])
        kv = _nn(a, wkv)
        k_s[rows, :] = turned(kv[:, :HEAD])
        v = kv[:, HEAD:].astype(BF16)
        v_s[rows, :] = v
        vt_s[:HEAD, rows] = v.T
        for g in range(HEADS):
            s = _nt(k_s[:keys, :], q_s[g, rows, :])
            own = _hide(s[i * STRIP :, :], 0, 0)
            s = own if i == 0 else jnp.concatenate([s[: i * STRIP, :], own], axis=0)
            top = jnp.max(s, axis=0, keepdims=True)
            p = jnp.exp2((s - top) * (SCALE * LOG2E)).astype(BF16)
            mix = _nn(vt_s[:, :keys], p)
            total = mix[HEAD : HEAD + 1, :]
            o_s[rows, _lanes(g)] = (mix[:HEAD, :] * (1 / total)).T.astype(BF16)
            lse_s[g, :, rows] = top * (SCALE * LOG2E) + jnp.log2(total)
        h = (x + _nn(o_s[rows, :], wo_ref[...]).astype(BF16).astype(F32)).astype(BF16)
        h_s[rows, :] = h
        h = h.astype(F32)
        b = (h * _scale(h)).astype(BF16)
        b_s[rows, :] = b
        bt_s[:, rows] = b.T
        for src, dst in zip(held, outs, strict=True):
            if src is q_s:
                src, dst = src.at[:, rows, :], dst.at[:, rows, :]
            elif src is bt_s:
                src, dst = src.at[:, rows], dst.at[:, rows]
            elif src is lse_s:
                src, dst = src.at[:, :, rows], dst.at[:, :, rows]
            else:
                src, dst = src.at[rows, :], dst.at[rows, :]
            copies.append(pltpu.make_async_copy(src, dst, sem.at[len(copies)]))
            copies[-1].start()
    for copy in copies:
        copy.wait()


def _params(**more):
    return pltpu.CompilerParams(vmem_limit_bytes=VMEM, **more)


def _turns():
    angle = np.arange(TOKENS)[:, None] * float(THETA) ** (-np.arange(HALF) / HALF)
    return jnp.asarray(np.concatenate([np.cos(angle), np.sin(angle)], 1), F32)


ANYWHERE = pl.BlockSpec(memory_space=pl.ANY)
IN_VMEM = pl.BlockSpec(memory_space=pltpu.VMEM)


def front(x, turns, wq, wk, wv, wo):
    shapes = [((HEADS, TOKENS, HEAD), BF16), ((TOKENS, HEAD), BF16), ((TOKENS, HEAD), BF16), ((TOKENS, D), BF16), ((TOKENS, D), BF16),
              ((TOKENS, D), BF16), ((D, TOKENS), BF16), ((HEADS, 1, TOKENS), F32)]
    return pl.pallas_call(
        _front,
        in_specs=[IN_VMEM] * 6,
        out_specs=[ANYWHERE] * 8,
        out_shape=[jax.ShapeDtypeStruct(*one) for one in shapes],
        scratch_shapes=[pltpu.VMEM(*one) for one in shapes] + [pltpu.VMEM((HEAD + 8, TOKENS), BF16), pltpu.SemaphoreType.DMA((32,))],
        compiler_params=_params(),
        cost_estimate=pl.CostEstimate(flops=5 * 10**9, transcendentals=4 * 10**6, bytes_accessed=15 * 10**6),
        name="front",
    )(x, turns, wq, wk, wv, wo)


class _Links:
    def __init__(self):
        me = lax.axis_index("dp")
        self.at = [lax.rem(lax.div(me, stride), SIDE) for stride in STRIDES]
        self.core = lax.rem(me, 2)
        self.partner = me + 1 - 2 * self.core

        def along(d, q):
            return me + STRIDES[d] * (lax.rem(self.at[d] + q, SIDE) - self.at[d])

        self.plus, self.minus = ([along(d, q) for d in range(3)] for q in (NEXT, LAST))

    def greet(self):
        barrier = pltpu.get_barrier_semaphore()
        others = (*self.plus, *self.minus, self.partner)
        for other in others:
            pl.semaphore_signal(barrier, inc=1, device_id={"dp": other}, device_id_type=pl.DeviceIdType.MESH)
        pl.semaphore_wait(barrier, len(others))

    def position(self, k, dim, q):
        return lax.rem(self.at[ORDERS[k][dim]] + q, SIDE)


def _remote(src, dst, send_sem, recv_sem, other):
    return pltpu.make_async_remote_copy(src_ref=src, dst_ref=dst, send_sem=send_sem, recv_sem=recv_sem, device_id={"dp": other},
                                        device_id_type=pl.DeviceIdType.MESH)


def _mlp(b_ref, bt_ref, dy_ref, wg_ref, wu_ref, wd_ref, sum_ref, db_ref, acc, g_s, r_s, lo_s, hi_s, two_s, ssem, rsem):
    f = pl.program_id(0)
    links = _Links()
    mine, theirs = links.core * PER_CORE, (1 - links.core) * PER_CORE
    low, high = slice(0, LOW), slice(LOW, WAVE)

    def pair(u):
        return _remote(g_s.at[u, pl.ds(theirs, PER_CORE)], r_s.at[u], ssem.at[u, 0], rsem.at[u, 0], links.partner)

    def message(u, k, n):
        d, back = ORDERS[k][0], n % 2
        rows = (low, high)[n in (1, 2, 5)]
        src = g_s.at[u, mine + SIDE * k + links.position(k, 0, FAR if n < 2 else (NEXT, LAST)[back]), rows]
        dst = (lo_s, hi_s)[n].at[u, k] if n < 2 else two_s.at[u, k, back, rows]
        return _remote(src, dst, ssem.at[u, 6 * k + n + 1], rsem.at[u, 6 * k + n + 1], (links.minus if back else links.plus)[d])

    def both(u, k, q, rows):
        j = SIDE * k + links.position(k, 0, q)
        return g_s[u, mine + j, rows, :].astype(F32) + r_s[u, j, rows, :].astype(F32)

    def put(u, k, q, rows, total):
        g_s[u, mine + SIDE * k + links.position(k, 0, q), rows, :] = total.astype(BF16)

    def stage(lag):
        u = f - lag
        return lambda run: pl.when((u >= 0) & (u < WAVES))(lambda: run(u))

    @pl.when(f == 0)
    def _():
        links.greet()

    @stage(4)
    def _(u):
        for k in COLOURS:
            for n in range(2, 6):
                message(u, k, n).wait_recv()
            for rows in (low, high):
                here = pl.ds(pl.multiple_of(u * WAVE + rows.start, TILE), rows.stop - rows.start)
                sum_ref[k, here, :] = both(u, k, 0, rows) + two_s[u, k, 0, rows, :].astype(F32) + two_s[u, k, 1, rows, :].astype(F32)

    @stage(3)
    def _(u):
        for k in COLOURS:
            message(u, k, 0).wait_recv()
            put(u, k, NEXT, low, both(u, k, NEXT, low) + lo_s[u, k].astype(F32))
            message(u, k, 4).start()
            message(u, k, 1).wait_recv()
            put(u, k, LAST, high, both(u, k, LAST, high) + hi_s[u, k].astype(F32))
            message(u, k, 5).start()

    @stage(2)
    def _(u):
        pair(u).wait_recv()
        for k in COLOURS:
            for n, (q, rows) in enumerate(((FAR, low), (FAR, high), (NEXT, high), (LAST, low))):
                put(u, k, q, rows, both(u, k, q, rows))
                message(u, k, n).start()

    @pl.when(f < WAVES)
    def _():
        wgu = jnp.concatenate([wg_ref[...], wu_ref[...]], axis=1)
        gu = _nn(b_ref[...], wgu)
        gate, up = gu[:, :BLOCK], gu[:, BLOCK:]
        dact = _nt(dy_ref[...], wd_ref[...]).astype(BF16).astype(F32)
        s = 0.5 * jnp.tanh(0.5 * gate) + 0.5
        silu = gate * s
        act = (silu * up).astype(BF16)
        dgu = jnp.concatenate([(dact * up * (s + silu * (1 - s))).astype(BF16), (dact * silu).astype(BF16)], axis=1)
        dw = _nn(bt_ref[...], dgu).astype(BF16)
        dwd = _dot(act, dy_ref[...], 0, 0).astype(BF16)
        for r in range(8):
            j = r // SIDE * PER_CORE + r % SIDE
            for n in range(6):
                g_s[f, j + n // 3 * SIDE, _span(n % 3, EIGHTH), :] = dw[_span(r, EIGHTH), _lanes(n)]
            for t in range(HEADS):
                g_s[f, j + 2 * SIDE, _span(t, DOWN), :] = dwd[_span(r, DOWN), _lanes(t)]
        acc[...] = jnp.where(f > 0, acc[...], 0.0) + _nt(dgu, wgu)
        pair(f).start()

    @pl.when(f == WAVES - 1)
    def _():
        db_ref[...] = acc[...].astype(BF16)

    @pl.when(f == WAVES + 3)
    def _():
        @pl.loop(0, WAVES)
        def _(u):
            for copy in (pair(u), *(message(u, k, n) for k in COLOURS for n in range(6))):
                copy.wait_send()


def mlp(b, bt, dy, wg, wu, wd):
    vmem = lambda *shape: pltpu.VMEM((*shape, LANES), BF16)
    whole = lambda *shape: pl.BlockSpec(shape, lambda f: (0,) * len(shape), pipeline_mode=pl.Buffered(1))
    across = pl.BlockSpec((D, BLOCK), lambda f: (0, jnp.minimum(f, WAVES - 1)))
    down = pl.BlockSpec((BLOCK, D), lambda f: (jnp.minimum(f, WAVES - 1), 0))
    sems = pltpu.SemaphoreType.DMA((WAVES, 19))
    return pl.pallas_call(
        _mlp,
        grid=(WAVES + 4,),
        in_specs=[whole(TOKENS, D), whole(D, TOKENS), whole(TOKENS, D), across, across, down],
        out_specs=[whole(3, MLP, LANES), whole(TOKENS, D)],
        out_shape=[jax.ShapeDtypeStruct((3, MLP, LANES), F32), jax.ShapeDtypeStruct((TOKENS, D), BF16)],
        scratch_shapes=[pltpu.VMEM((TOKENS, D), F32), vmem(WAVES, PIECES, WAVE), vmem(WAVES, PER_CORE, WAVE), vmem(WAVES, 3, LOW),
                        vmem(WAVES, 3, WAVE - LOW), vmem(WAVES, 3, 2, WAVE), sems, sems],
        compiler_params=_params(dimension_semantics=("arbitrary",), collective_id=1, has_side_effects=True),
        cost_estimate=pl.CostEstimate(flops=16 * TOKENS * D * FF, transcendentals=TOKENS * FF, bytes_accessed=40 * 2**20),
        name="mlp",
    )(b, bt, dy, wg, wu, wd)


def _back(x_ref, dy_ref, db_ref, h_ref, q_ref, k_ref, v_ref, o_ref, lse_ref, turns_ref, wo_ref, ga_ref,
          at_s, ot_s, dh_s, do_s, delta_s, kt_s, dq_s, dk_s, dv_s):
    strips = range(TOKENS // STRIP)
    kt_s[...] = k_ref[...].T
    dk_s[...] = jnp.zeros_like(dk_s)
    dv_s[...] = jnp.zeros_like(dv_s)

    def turned_back(t, rows):
        t = t.astype(BF16).astype(F32)
        cos, sin = _turning(turns_ref, rows)
        return (t * cos + pltpu.roll(t * sin, HALF, 1)).astype(BF16)

    for i in strips:
        rows = _span(i, STRIP)
        keys = rows.stop
        h, db = h_ref[rows, :].astype(F32), db_ref[rows, :].astype(F32)
        scale = _scale(h)
        by_scale = jnp.sum(db * h, -1, keepdims=True)
        dh = (db * scale - h * (by_scale * scale * scale * scale * (1 / D))).astype(BF16).astype(F32)
        dh = (dy_ref[rows, :].astype(F32) + dh).astype(BF16)
        dh_s[rows, :] = dh
        do = _nt(dh, wo_ref[...]).astype(BF16)
        o = o_ref[rows, :]
        ot_s[:, rows] = o.T
        x = x_ref[rows, :].astype(F32)
        at_s[:, rows] = (x * _scale(x)).astype(BF16).T
        for g in range(HEADS):
            do_s[g, rows, :] = do[:, _lanes(g)]
            both = do[:, _lanes(g)].astype(F32) * o[:, _lanes(g)].astype(F32)
            delta_s[g, :, rows] = jnp.sum(both.T, axis=0, keepdims=True)

        def head(g):
            q, do_g = q_ref[g, rows, :], do_s[g, rows, :]
            s = _nt(k_ref[:keys, :], q)
            own = _hide(s[i * STRIP :, :], 0, 0)
            s = own if i == 0 else jnp.concatenate([s[: i * STRIP, :], own], axis=0)
            p = jnp.exp2(s * (SCALE * LOG2E) - lse_ref[g, :, rows])
            ds = (p * (_nt(v_ref[:keys, :], do_g) - delta_s[g, :, rows])).astype(BF16)
            dv_s[:keys, :] += _nn(p.astype(BF16), do_g)
            dk_s[:keys, :] += _nn(ds, q)
            dq = (_nn(kt_s[:, :keys], ds) * SCALE).T
            dq_s[g, rows, :] = turned_back(dq, rows)

        pl.loop(0, HEADS)(head)

    every = slice(None)
    dqkv = [dq_s[g] for g in range(HEADS)] + [turned_back(dk_s[...] * SCALE, every), dv_s[...].astype(BF16)]
    dqkv = _nn(at_s[...], jnp.concatenate(dqkv, axis=1)).astype(BF16)
    dwo = _nn(ot_s[...], dh_s[...]).astype(BF16)
    for r in range(8):
        j, rows = r // 4 * PER_CORE + r % 4, _span(r, EIGHTH)
        for t in range(HEADS):
            here = _span(t, EIGHTH)
            ga_ref[j, here, :] = dqkv[rows, _lanes(t)]
            ga_ref[j + 4, here, :] = dwo[rows, _lanes(t)]
            ga_ref[j + 8, here, :] = dqkv[rows, _lanes(HEADS + t)] if t < 2 else jnp.zeros((EIGHTH, LANES), BF16)


def back(x, dy, db, h, q, k, v, o, lse, turns, wo):
    vmem = lambda *shape: pltpu.VMEM(shape, BF16)
    return pl.pallas_call(
        _back,
        in_specs=[IN_VMEM] * 11,
        out_specs=IN_VMEM,
        out_shape=jax.ShapeDtypeStruct((PIECES, ATTN, LANES), BF16),
        scratch_shapes=[vmem(D, TOKENS), vmem(D, TOKENS), vmem(TOKENS, D), vmem(HEADS, TOKENS, HEAD), pltpu.VMEM((HEADS, 1, TOKENS), F32),
                        vmem(HEAD, TOKENS), vmem(HEADS, TOKENS, HEAD), pltpu.VMEM((TOKENS, HEAD), F32), pltpu.VMEM((TOKENS, HEAD), F32)],
        compiler_params=_params(),
        cost_estimate=pl.CostEstimate(flops=8 * 10**9, transcendentals=4 * 10**6, bytes_accessed=15 * 10**6),
        name="back",
    )(x, dy, db, h, q, k, v, o, lse, turns, wo)


def _reduce(sum_ref, ga, out_m, out_a, nrm, aa, ra, a1, a2, s1, r1, t1, s2, r2, t2, s3, r3, t3, w, w2, ns, nd, ssem, rsem, lsem):
    links = _Links()
    at, core, partner = links.at, links.core, links.partner
    locals_, sent = [], []

    def send(src, dst, other):
        n = len(sent)
        sent.append(_remote(src, dst, ssem.at[n], rsem.at[n], other))
        sent[n].start()
        return sent[n]

    def local(src, dst):
        n = len(locals_)
        locals_.append(pltpu.make_async_copy(src, dst, lsem.at[n]))
        locals_[n].start()
        return locals_[n]

    mine, theirs = core * PER_CORE, (1 - core) * PER_CORE
    load = [local(ga.at[pl.ds(mine, PER_CORE)], aa), *(local(sum_ref.at[k], a1.at[k, :MLP]) for k in COLOURS)]
    links.greet()
    other_half = send(ga.at[pl.ds(theirs, PER_CORE)], ra, partner)

    def spread(rows, run):
        part = rows if rows < 256 else math.gcd(rows, 160)

        @pl.loop(0, rows // part)
        def _(i):
            run(pl.multiple_of(i * part, TILE), part)

    def ring(dim, size, low, term, s, first, second, store):
        high = size - low
        relays, plain, rest = {}, {}, {}

        def fill(k, slot, q, start, n, more=None):
            def run(i, part):
                total = term(k, links.position(k, dim, q), start + i, part)
                if more is not None:
                    total += first[k, more, pl.ds(i, part), :].astype(F32)
                s[k, slot, pl.ds(pl.multiple_of(start + i, TILE), part), :] = total.astype(BF16)

            spread(n, run)

        for k in COLOURS:
            plus, minus = (side[ORDERS[k][dim]] for side in (links.plus, links.minus))
            fill(k, 0, FAR, 0, low)
            relays[k] = [send(s.at[k, 0, :low], first.at[k, 0, :low], plus)]
            fill(k, 0, FAR, low, high)
            relays[k] += [send(s.at[k, 0, low:], first.at[k, 1, :high], minus)]
            fill(k, 1, NEXT, low, high)
            plain[k] = [send(s.at[k, 1, low:], second.at[k, 0, low:], plus)]
            fill(k, 2, LAST, 0, low)
            plain[k] += [send(s.at[k, 2, :low], second.at[k, 1, :low], minus)]
        for k in COLOURS:
            plus, minus = (side[ORDERS[k][dim]] for side in (links.plus, links.minus))
            relays[k][0].wait_recv()
            fill(k, 1, NEXT, 0, low, 0)
            rest[k] = [send(s.at[k, 1, :low], second.at[k, 0, :low], plus)]
            relays[k][1].wait_recv()
            fill(k, 2, LAST, low, high, 1)
            rest[k] += [send(s.at[k, 2, low:], second.at[k, 1, low:], minus)]
        for k in COLOURS:
            for copy in plain[k] + rest[k]:
                copy.wait_recv()

            def run(i, part):
                here = pl.ds(i, part)
                store(k, i, part, term(k, links.position(k, dim, 0), i, part) + second[k, 0, here, :].astype(F32) + second[k, 1, here, :].astype(F32))

            spread(size, run)

    def attention(k, place, start, n):
        here = (SIDE * k + place, pl.ds(start, n))
        return aa[here].astype(F32) + ra[here].astype(F32)

    def keep(ref, offset):
        def store(k, i, n, total):
            ref[k, pl.ds(pl.multiple_of(offset + i, TILE), n), :] = total

        return store

    def held(ref, size):
        return lambda k, place, start, n: ref[k, pl.ds(pl.multiple_of(place * size + start, TILE), n), :]

    def finish(k, i, n, total):
        rounded = total.astype(BF16)
        w[SIDE * k + links.position(k, 0, 0), pl.ds(pl.multiple_of(links.position(k, 1, 0) * Q2 + links.position(k, 2, 0) * Q3 + i, TILE), n), :] = rounded
        again = rounded.astype(F32)
        ns[2, at[2]] += jnp.sum((again * again).reshape(-1, 8, LANES), axis=0)

    load[0].wait()
    other_half.wait_recv()
    ring(0, ATTN, 208, attention, s1, r1, t1, keep(a1, MLP))
    for copy in load[1:]:
        copy.wait()
    ns[2, at[2]] = jnp.zeros((8, LANES), F32)
    ring(1, Q2, Q2 // 2, held(a1, Q2), s2, r2, t2, keep(a2, 0))
    ring(2, Q3, Q3 // 2, held(a2, Q3), s3, r3, t3, finish)

    def squares(d, q, other):
        slot = ns.at[d, lax.rem(at[d] + q, SIDE)]
        return send(slot, slot, other[d])

    given, out_copies = [], []

    def out(src, j):
        for rows, dst in ((slice(0, MLP), out_m), (slice(MLP, ROWS), out_a)):
            out_copies.append(local(src.at[rows], dst.at[j]))

    def finished(k, q):
        j = SIDE * k + links.position(k, 0, q)
        out(w.at[j], mine + j)
        given.append((send(w.at[j], w2.at[j], partner), j))

    for dim, size in ((2, Q3), (1, Q2), (0, ROWS)):
        half = size // 2

        def rows(k, q, start):
            base = {2: links.position(k, 1, 0) * Q2, 1: 0, 0: 0}[dim] + (links.position(k, dim, q) * size if dim else 0)
            return w.at[SIDE * k + links.position(k, 0, 0 if dim else q), pl.ds(pl.multiple_of(base + start, TILE), half)]

        ahead, behind, last = {}, {}, {}
        for k in COLOURS:
            plus, minus = (side[ORDERS[k][dim]] for side in (links.plus, links.minus))
            ahead[k] = [send(rows(k, 0, start), rows(k, 0, start), plus) for start in (0, half)]
            behind[k] = [send(rows(k, 0, start), rows(k, 0, start), minus) for start in (half, 0)]
        squared = [squares(dim, 0, links.plus), squares(dim, 0, links.minus)]
        for k in COLOURS:
            plus, minus = (side[ORDERS[k][dim]] for side in (links.plus, links.minus))
            ahead[k][0].wait_recv()
            last[k] = [send(rows(k, LAST, 0), rows(k, LAST, 0), plus)]
            behind[k][0].wait_recv()
            last[k] += [send(rows(k, NEXT, half), rows(k, NEXT, half), minus)]
            if dim == 0:
                finished(k, 0)
        for copy in squared:
            copy.wait_recv()
        squared = squares(dim, LAST, links.plus)
        for k in COLOURS:
            ahead[k][1].wait_recv()
            behind[k][1].wait_recv()
            if dim == 0:
                finished(k, LAST)
                finished(k, NEXT)
        squared.wait_recv()
        total = ns[dim, 0] + ns[dim, 1] + ns[dim, 2] + ns[dim, 3]
        if dim:
            ns[dim - 1, at[dim - 1]] = total
        else:
            nd[core] = total
            squared = send(nd.at[core], nd.at[core], partner)
        for k in COLOURS:
            for copy in last[k]:
                copy.wait_recv()
            if dim == 0:
                finished(k, FAR)
    for copy, j in given:
        copy.wait_recv()
        out(w2.at[j], theirs + j)
    squared.wait_recv()
    nrm[...] = nd[0] + nd[1]
    for copy in out_copies:
        copy.wait()
    for copy in sent:
        copy.wait_send()


def reduce_all(sums, ga):
    vmem = lambda *shape: pltpu.VMEM((*shape, LANES), BF16)
    wide = lambda *shape: pltpu.VMEM((*shape, LANES), F32)
    staged = [vmem(3, n, rows) for size in (ATTN, Q2, Q3) for n, rows in ((3, size), (2, 208 if size == ATTN else size // 2), (2, size))]
    many = pltpu.SemaphoreType.DMA((160,))
    return pl.pallas_call(
        _reduce,
        in_specs=[ANYWHERE] * 2,
        out_specs=[ANYWHERE] * 2 + [IN_VMEM],
        out_shape=[jax.ShapeDtypeStruct((PIECES, MLP, LANES), BF16), jax.ShapeDtypeStruct((PIECES, ATTN, LANES), BF16),
                   jax.ShapeDtypeStruct((8, LANES), F32)],
        scratch_shapes=[vmem(PER_CORE, ATTN), vmem(PER_CORE, ATTN), wide(3, ROWS), wide(3, Q2), *staged,
                        vmem(PER_CORE, ROWS), vmem(PER_CORE, ROWS), wide(3, SIDE, 8), wide(2, 8), many, many, many],
        compiler_params=_params(collective_id=0, has_side_effects=True),
        cost_estimate=pl.CostEstimate(flops=10**8, transcendentals=0, bytes_accessed=64 * 2**20),
        name="reduce_all",
    )(sums, ga)


def adamw(w, m, v, g):
    m = 0.9 * m + 0.1 * g
    v = 0.95 * v + 0.05 * g * g
    step = m * lax.rsqrt(v + 1e-8) + 0.1 * w
    return (w - 0.02 * step).astype(BF16), m, v


THIRD = WAVES // 3


def _adam(nrm_ref, gm_ref, ga_ref, *refs):
    total = jnp.sum(jnp.sum(nrm_ref[...], axis=0, keepdims=True), axis=1, keepdims=True)
    factor = jnp.minimum(1.0, 0.5 * lax.rsqrt(total / (3 * D * FF + 2 * D * (D + HEAD)) + 1e-30))
    wq, wk, wv, wo, gate, up, down = (refs[i::7] for i in range(7))

    def step(refs, where, g):
        w, m, v, new_w, new_m, new_v = refs
        new_w[where], new_m[where], new_v[where] = adamw(w[where].astype(F32), m[where], v[where], g.astype(F32) * factor)

    for n in range(THIRD):
        for t in range(3):
            here = _span(3 * n + t, EIGHTH)
            for k, refs in enumerate((gate, up)):
                step(refs, (slice(None), _lanes(3 * n + t)), gm_ref[0, k, 0, here, :])
        for t in range(5):
            here = _span(5 * n + t, DOWN)
            step(down, (n, 0, slice(None), _lanes(t)), gm_ref[0, 2, 0, here, :])

    @pl.when(pl.program_id(1) == 2)
    def _():
        for k, refs in enumerate((wq, wo)):
            for t in range(HEADS):
                step(refs, (slice(None), _lanes(t)), ga_ref[0, k, 0, _span(t, EIGHTH), :])
        for t, refs in enumerate((wk, wv)):
            step(refs, (slice(None), slice(None)), ga_ref[0, 2, 0, _span(t, EIGHTH), :])


def adam(nrm, gm, ga, *wmv):
    small = lambda width: pl.BlockSpec((EIGHTH, width), lambda r, i: (r, 0))
    across = pl.BlockSpec((EIGHTH, THIRD * BLOCK), lambda r, i: (r, i))
    specs = [small(D), small(HEAD), small(HEAD), small(D), across, across, pl.BlockSpec((THIRD, 1, DOWN, D), lambda r, i: (i, r, 0, 0))] * 3
    given = [one.reshape(WAVES, 8, DOWN, D) if one.shape[0] == FF else one for one in wmv]
    pieces = lambda g: g.reshape(2, 3, 4, -1, LANES)
    got = pl.pallas_call(
        _adam,
        grid=(8, 3),
        in_specs=[
            pl.BlockSpec((8, LANES), lambda r, i: (0, 0)),
            pl.BlockSpec((1, 3, 1, THIRD * WAVE, LANES), lambda r, i: (r // 4, 0, r % 4, i, 0)),
            pl.BlockSpec((1, 3, 1, ATTN, LANES), lambda r, i: (r // 4, 0, r % 4, 0, 0)),
            *specs,
        ],
        out_specs=specs,
        out_shape=[jax.ShapeDtypeStruct(one.shape, one.dtype) for one in given],
        compiler_params=_params(dimension_semantics=("arbitrary", "arbitrary")),
        cost_estimate=pl.CostEstimate(flops=10**8, transcendentals=8 * 10**6, bytes_accessed=168 * 10**6),
        name="adam",
    )(nrm, pieces(gm), pieces(ga), *given)
    return [one.reshape(was.shape) for one, was in zip(got, wmv, strict=True)]


def solution(mesh):
    def step(x, dy, *arrays):
        x, dy = x[0], dy[0]
        given = [one[0] for one in arrays]
        wq, wk, wv, wo, gate, up, down = given[:7]
        turns = _turns()
        q, k, v, o, h, b, bt, lse = front(x, turns, wq, wk, wv, wo)
        sums, db = mlp(b, bt, dy, gate, up, down)
        ga = back(x, dy, db, h, q, k, v, o, lse, turns, wo)
        gm, ga, nrm = reduce_all(sums, ga)
        return tuple(one[None] for one in adam(nrm, gm, ga, *given))

    states, all_of = P(("rep", "dp"), None, None), P(None, None, None)
    return jax.shard_map(
        step,
        mesh=mesh,
        in_specs=(states, states) + (all_of,) * 21,
        out_specs=(P("rep", None, None),) * 21,
        check_vma=False,
    )
```

```python
import jax
import jax.numpy as jnp
import numpy as np
from jax import lax
from jax.experimental import pallas as pl
from jax.experimental.pallas import tpu as pltpu
from jax.sharding import PartitionSpec as P

BF16, F32 = jnp.bfloat16, jnp.float32
LANES = 128
TOKENS, D, HEADS, FF = 1024, 640, 5, 3456
HEAD, HALF = LANES, LANES // 2
THETA = 10000
HIDDEN = -1e30
SCALE = HEAD**-0.5
LOG2E = 1.4426950408889634
VMEM = 56 * 2**20
STRIP = 256
EIGHTH, DOWN = 80, 48
WAVES, BLOCK = 9, 384
WAVE, ATTN = 240, 400
MLP = WAVES * WAVE
STEPS = ((MLP, 576), (ATTN, 128))
LOW = 128
SIDE = 4
SLOTS = 5
NEXT, FAR, LAST = 1, 2, 3
PADDED = tuple(SIDE * rows for _, rows in STEPS)
STRIDES = (32, 8, 2)
ORDERS = ((0, 1, 2), (1, 2, 0), (2, 0, 1))
COLOURS = range(3)
TILE = 16
PER_CORE, PIECES = 12, 24


def _dot(a, b, ca, cb):
    return lax.dot_general(a, b, (((ca,), (cb,)), ((), ())), preferred_element_type=F32)


def _nn(a, b):
    return _dot(a, b, 1, 0)


def _nt(a, b):
    return _dot(a, b, 1, 1)


def _scale(wide):
    return lax.rsqrt(jnp.mean(wide * wide, -1, keepdims=True) + 1e-6)


def _span(n, size):
    return slice(n * size, n * size + size)


def _lanes(n):
    return _span(n, LANES)


def _turning(turns_ref, rows):
    table = turns_ref[rows, :]
    other = pltpu.roll(table, HALF, 1)
    first = lax.broadcasted_iota(jnp.int32, table.shape, 1) < HALF
    return jnp.where(first, table, other), jnp.where(first, -other, table)


def _hide(s, first_key, first_query):
    key = lax.broadcasted_iota(jnp.int32, s.shape, 0) + first_key
    query = lax.broadcasted_iota(jnp.int32, s.shape, 1) + first_query
    return jnp.where(query >= key, s, HIDDEN)


def _front(x_ref, turns_ref, wq_ref, wk_ref, wv_ref, wo_ref, *rest):
    outs, held, (vt_s, sem) = rest[:8], rest[8:16], rest[16:]
    q_s, k_s, v_s, o_s, h_s, b_s, bt_s, lse_s = held
    copies = []
    wkv = jnp.concatenate([wk_ref[...], wv_ref[...]], axis=1)
    vt_s[HEAD:, :] = jnp.ones((vt_s.shape[0] - HEAD, TOKENS), BF16)
    for i in range(TOKENS // STRIP):
        rows = _span(i, STRIP)
        keys = rows.stop
        x = x_ref[rows, :].astype(F32)
        a = (x * _scale(x)).astype(BF16)
        cos, sin = _turning(turns_ref, rows)

        def turned(t):
            t = t.astype(BF16).astype(F32)
            return (t * cos + pltpu.roll(t, HALF, 1) * sin).astype(BF16)

        q = _nn(a, wq_ref[...])
        for g in range(HEADS):
            q_s[g, rows, :] = turned(q[:, _lanes(g)])
        kv = _nn(a, wkv)
        k_s[rows, :] = turned(kv[:, :HEAD])
        v = kv[:, HEAD:].astype(BF16)
        v_s[rows, :] = v
        vt_s[:HEAD, rows] = v.T
        for g in range(HEADS):
            s = _nt(k_s[:keys, :], q_s[g, rows, :])
            own = _hide(s[i * STRIP :, :], 0, 0)
            s = own if i == 0 else jnp.concatenate([s[: i * STRIP, :], own], axis=0)
            top = jnp.max(s, axis=0, keepdims=True)
            p = jnp.exp2((s - top) * (SCALE * LOG2E)).astype(BF16)
            mix = _nn(vt_s[:, :keys], p)
            total = mix[HEAD : HEAD + 1, :]
            o_s[rows, _lanes(g)] = (mix[:HEAD, :] * (1 / total)).T.astype(BF16)
            lse_s[g, :, rows] = top * (SCALE * LOG2E) + jnp.log2(total)
        h = (x + _nn(o_s[rows, :], wo_ref[...]).astype(BF16).astype(F32)).astype(BF16)
        h_s[rows, :] = h
        h = h.astype(F32)
        b = (h * _scale(h)).astype(BF16)
        b_s[rows, :] = b
        bt_s[:, rows] = b.T
        for src, dst in zip(held, outs, strict=True):
            if src is q_s:
                src, dst = src.at[:, rows, :], dst.at[:, rows, :]
            elif src is bt_s:
                src, dst = src.at[:, rows], dst.at[:, rows]
            elif src is lse_s:
                src, dst = src.at[:, :, rows], dst.at[:, :, rows]
            else:
                src, dst = src.at[rows, :], dst.at[rows, :]
            copies.append(pltpu.make_async_copy(src, dst, sem.at[len(copies)]))
            copies[-1].start()
    for copy in copies:
        copy.wait()


def _params(**more):
    return pltpu.CompilerParams(vmem_limit_bytes=VMEM, **more)


def _turns():
    angle = np.arange(TOKENS)[:, None] * float(THETA) ** (-np.arange(HALF) / HALF)
    return jnp.asarray(np.concatenate([np.cos(angle), np.sin(angle)], 1), F32)


ANYWHERE = pl.BlockSpec(memory_space=pl.ANY)
IN_VMEM = pl.BlockSpec(memory_space=pltpu.VMEM)


def front(x, turns, wq, wk, wv, wo):
    shapes = [((HEADS, TOKENS, HEAD), BF16), ((TOKENS, HEAD), BF16), ((TOKENS, HEAD), BF16), ((TOKENS, D), BF16), ((TOKENS, D), BF16),
              ((TOKENS, D), BF16), ((D, TOKENS), BF16), ((HEADS, 1, TOKENS), F32)]
    return pl.pallas_call(
        _front,
        in_specs=[IN_VMEM] * 6,
        out_specs=[ANYWHERE] * 8,
        out_shape=[jax.ShapeDtypeStruct(*one) for one in shapes],
        scratch_shapes=[pltpu.VMEM(*one) for one in shapes] + [pltpu.VMEM((HEAD + 8, TOKENS), BF16), pltpu.SemaphoreType.DMA((32,))],
        compiler_params=_params(),
        cost_estimate=pl.CostEstimate(flops=5 * 10**9, transcendentals=4 * 10**6, bytes_accessed=15 * 10**6),
        name="front",
    )(x, turns, wq, wk, wv, wo)


class _Links:
    def __init__(self):
        me = lax.axis_index("dp")
        self.at = [lax.rem(lax.div(me, stride), SIDE) for stride in STRIDES]
        self.core = lax.rem(me, 2)
        self.partner = me + 1 - 2 * self.core

        def along(d, q):
            return me + STRIDES[d] * (lax.rem(self.at[d] + q, SIDE) - self.at[d])

        self.plus, self.minus = ([along(d, q) for d in range(3)] for q in (NEXT, LAST))

    def greet(self):
        for other in (*self.plus, *self.minus, self.partner):
            pl.semaphore_signal(pltpu.get_barrier_semaphore(), inc=1, device_id={"dp": other}, device_id_type=pl.DeviceIdType.MESH)

    def met(self):
        pl.semaphore_wait(pltpu.get_barrier_semaphore(), 7)

    def position(self, k, dim, q):
        return lax.rem(self.at[ORDERS[k][dim]] + q, SIDE)


def _remote(src, dst, send_sem, recv_sem, other):
    return pltpu.make_async_remote_copy(src_ref=src, dst_ref=dst, send_sem=send_sem, recv_sem=recv_sem, device_id={"dp": other},
                                        device_id_type=pl.DeviceIdType.MESH)


def _mlp(b_ref, bt_ref, dy_ref, wg_ref, wu_ref, wd_ref, sum_ref, db_ref, acc, g_s, r_s, lo_s, hi_s, two_s, ssem, rsem):
    f = pl.program_id(0)
    links = _Links()
    mine, theirs = links.core * PER_CORE, (1 - links.core) * PER_CORE
    low, high = slice(0, LOW), slice(LOW, WAVE)

    def pair(u):
        return _remote(g_s.at[u, pl.ds(theirs, PER_CORE)], r_s.at[u], ssem.at[u % SLOTS], rsem.at[u % SLOTS, 0], links.partner)

    def message(u, k, n):
        d, back = ORDERS[k][0], n % 2
        rows = (low, high)[n in (1, 2, 5)]
        src = g_s.at[u, mine + SIDE * k + links.position(k, 0, FAR if n < 2 else (NEXT, LAST)[back]), rows]
        dst = (lo_s, hi_s)[n].at[u, k] if n < 2 else two_s.at[u, k, back, rows]
        return _remote(src, dst, ssem.at[u % SLOTS], rsem.at[u % SLOTS, 6 * k + n + 1], (links.minus if back else links.plus)[d])

    def both(u, k, q, rows):
        j = SIDE * k + links.position(k, 0, q)
        return g_s[u, mine + j, rows, :].astype(F32) + r_s[u, j, rows, :].astype(F32)

    def put(u, k, q, rows, total):
        g_s[u, mine + SIDE * k + links.position(k, 0, q), rows, :] = total.astype(BF16)

    def stage(lag):
        u = f - lag
        return lambda run: pl.when((u >= 0) & (u < WAVES))(lambda: run(u))

    @pl.when(f == 0)
    def _():
        links.greet()

    @pl.when(f == 1)
    def _():
        links.met()

    @stage(1)
    def _(u):
        pair(u).start()

    @stage(2)
    def _(u):
        pair(u).wait_recv()
        for k in COLOURS:
            for n, (q, rows) in enumerate(((FAR, low), (FAR, high), (NEXT, high), (LAST, low))):
                put(u, k, q, rows, both(u, k, q, rows))
                message(u, k, n).start()

    @stage(3)
    def _(u):
        for k in COLOURS:
            message(u, k, 0).wait_recv()
            put(u, k, NEXT, low, both(u, k, NEXT, low) + lo_s[u, k].astype(F32))
            message(u, k, 4).start()
            message(u, k, 1).wait_recv()
            put(u, k, LAST, high, both(u, k, LAST, high) + hi_s[u, k].astype(F32))
            message(u, k, 5).start()

    @stage(4)
    def _(u):
        for k in COLOURS:
            for n in range(2, 6):
                message(u, k, n).wait_recv()
            for rows in (low, high):
                here = pl.ds(pl.multiple_of(u * WAVE + rows.start, TILE), rows.stop - rows.start)
                sum_ref[k, here, :] = both(u, k, 0, rows) + two_s[u, k, 0, rows, :].astype(F32) + two_s[u, k, 1, rows, :].astype(F32)
        sent = g_s.at[u, pl.ds(0, 21)]
        pltpu.make_async_copy(sent, sent, ssem.at[u % SLOTS]).wait()

    @pl.when(f < WAVES)
    def _():
        wgu = jnp.concatenate([wg_ref[...], wu_ref[...]], axis=1)
        gu = _nn(b_ref[...], wgu)
        gate, up = gu[:, :BLOCK], gu[:, BLOCK:]
        dact = _nt(dy_ref[...], wd_ref[...]).astype(BF16).astype(F32)
        s = 0.5 * jnp.tanh(0.5 * gate) + 0.5
        silu = gate * s
        act = (silu * up).astype(BF16)
        dgu = jnp.concatenate([(dact * up * (s + silu * (1 - s))).astype(BF16), (dact * silu).astype(BF16)], axis=1)
        dw = _nn(bt_ref[...], dgu).astype(BF16)
        dwd = _dot(act, dy_ref[...], 0, 0).astype(BF16)
        for r in range(8):
            j = r // SIDE * PER_CORE + r % SIDE
            for n in range(6):
                g_s[f, j + n // 3 * SIDE, _span(n % 3, EIGHTH), :] = dw[_span(r, EIGHTH), _lanes(n)]
            for t in range(HEADS):
                g_s[f, j + 2 * SIDE, _span(t, DOWN), :] = dwd[_span(r, DOWN), _lanes(t)]
        acc[...] = jnp.where(f > 0, acc[...], 0.0) + _nt(dgu, wgu)

    @pl.when(f == WAVES - 1)
    def _():
        db_ref[...] = acc[...].astype(BF16)

    @pl.when(f == WAVES + 3)
    def _():
        sum_ref[:, MLP:, :] = jnp.zeros((3, PADDED[0] - MLP, LANES), F32)


def mlp(b, bt, dy, wg, wu, wd):
    vmem = lambda *shape: pltpu.VMEM((*shape, LANES), BF16)
    whole = lambda *shape: pl.BlockSpec(shape, lambda f: (0,) * len(shape), pipeline_mode=pl.Buffered(1))
    across = pl.BlockSpec((D, BLOCK), lambda f: (0, jnp.minimum(f, WAVES - 1)))
    down = pl.BlockSpec((BLOCK, D), lambda f: (jnp.minimum(f, WAVES - 1), 0))
    return pl.pallas_call(
        _mlp,
        grid=(WAVES + 4,),
        in_specs=[whole(TOKENS, D), whole(D, TOKENS), whole(TOKENS, D), across, across, down],
        out_specs=[whole(3, PADDED[0], LANES), whole(TOKENS, D)],
        out_shape=[jax.ShapeDtypeStruct((3, PADDED[0], LANES), F32), jax.ShapeDtypeStruct((TOKENS, D), BF16)],
        scratch_shapes=[pltpu.VMEM((TOKENS, D), F32), vmem(WAVES, PIECES, WAVE), vmem(WAVES, PER_CORE, WAVE), vmem(WAVES, 3, LOW),
                        vmem(WAVES, 3, WAVE - LOW), vmem(WAVES, 3, 2, WAVE), pltpu.SemaphoreType.DMA((SLOTS,)), pltpu.SemaphoreType.DMA((SLOTS, 19))],
        compiler_params=_params(dimension_semantics=("arbitrary",), collective_id=1, has_side_effects=True),
        cost_estimate=pl.CostEstimate(flops=16 * TOKENS * D * FF, transcendentals=TOKENS * FF, bytes_accessed=40 * 2**20),
        name="mlp",
    )(b, bt, dy, wg, wu, wd)


class _Flow:
    def __init__(self, links, part, term, a1, a2, stage, w, out, ns, ssem, rsem, lsem):
        self.links, self.part, self.term, self.a1, self.a2, self.stage, self.w, self.out, self.ns = links, part, term, a1, a2, stage, w, out, ns
        self.ssem, self.rsem, self.lsem, self.received, self.groups = ssem, rsem, lsem, 0, 0
        self.rows = 0

    def send(self, src, dst, other, given=False):
        copy = _remote(src, dst, self.ssem.at[self.ssem.shape[0] - 1 if given else self.groups], self.rsem.at[self.received], other)
        copy.start()
        self.received += 1
        self.rows += 0 if given else src.size // LANES
        return copy

    def drain(self):
        sent = self.w.at[pl.ds(0, self.rows)]
        pltpu.make_async_copy(sent, sent, self.ssem.at[self.groups]).wait()
        self.groups += 1
        self.rows = 0

    def sides(self, k, dim):
        return (side[ORDERS[k][dim]] for side in (self.links.plus, self.links.minus))

    def ring(self, dim, size, term, stage, store):
        staged, first, second = stage
        low = first.shape[2]
        high = size - low
        position = self.links.position
        relays, rest = {}, {}

        def fill(k, slot, q, start, n, more=None):
            total = term(k, position(k, dim, q), start, n)
            if more is not None:
                total += first[k, more, :n, :].astype(F32)
            staged[k, slot, start : start + n, :] = total.astype(BF16)

        for k in COLOURS:
            plus, minus = self.sides(k, dim)
            fill(k, 0, FAR, 0, low)
            fill(k, 0, FAR, low, high)
            relays[k] = [self.send(staged.at[k, 0, :low], first.at[k, 0], plus), self.send(staged.at[k, 0, low:], first.at[k, 1, :high], minus)]
            fill(k, 1, NEXT, low, high)
            fill(k, 2, LAST, 0, low)
        yield
        for k in COLOURS:
            plus, minus = self.sides(k, dim)
            relays[k][0].wait_recv()
            fill(k, 1, NEXT, 0, low, 0)
            rest[k] = [self.send(staged.at[k, 1], second.at[k, 0], plus)]
            relays[k][1].wait_recv()
            fill(k, 2, LAST, low, high, 1)
            rest[k] += [self.send(staged.at[k, 2], second.at[k, 1], minus)]
        yield
        for k in COLOURS:
            for copy in rest[k]:
                copy.wait_recv()
            for start in range(0, size, low):
                here = slice(start, min(start + low, size))
                total = term(k, position(k, dim, 0), start, here.stop - start)
                store(k, start, total + second[k, 0, here, :].astype(F32) + second[k, 1, here, :].astype(F32))
        self.drain()

    def around(self, dim, block, size):
        low = -(-size // (2 * TILE)) * TILE
        first, second = {}, {}
        for k in COLOURS:
            first[k] = [self.send(block(k, 0, 0, size), block(k, 0, 0, size), side) for side in self.sides(k, dim)]
        yield
        for k in COLOURS:
            plus, minus = self.sides(k, dim)
            first[k][0].wait_recv()
            second[k] = [self.send(block(k, LAST, 0, low), block(k, LAST, 0, low), plus)]
            first[k][1].wait_recv()
            second[k] += [self.send(block(k, NEXT, low, size - low), block(k, NEXT, low, size - low), minus)]
        yield
        for k in COLOURS:
            for copy in second[k]:
                copy.wait_recv()
        self.drain()

    def run(self):
        position = self.links.position
        rows, size = STEPS[self.part]
        whole = PADDED[self.part]
        mine = self.links.core * PER_CORE
        given = []

        def keep(k, i, total):
            self.a1[k, i : i + total.shape[0], :] = total

        def held(k, place, start, n):
            return self.a1[k, pl.ds(pl.multiple_of(place * size + start, TILE), n), :]

        def third(k, i, total):
            self.a2[k, pl.ds(pl.multiple_of(position(k, 2, 0) * size + i, TILE), total.shape[0]), :] = total.astype(BF16)

        def terms(k, q, start, n):
            return self.a2.at[k, pl.ds(pl.multiple_of(position(k, 2, q) * size + start, TILE), n)]

        def row(k, piece, start, n):
            return pl.ds(pl.multiple_of((SIDE * k + piece) * whole + start, TILE), n)

        def second(k, q, start, n):
            return self.w.at[row(k, position(k, 0, 0), position(k, 1, q) * size + start, n)]

        def first(k, q, start, n):
            return self.w.at[row(k, position(k, 0, q), start, n)]

        def give(*distances):
            for q in distances:
                for k in COLOURS:
                    src, dst = first(k, q, 0, rows), self.out.at[mine + SIDE * k + position(k, 0, q)]
                    given.append(self.send(src, dst, self.links.partner, True))
                    pltpu.make_async_copy(src, dst, self.lsem).start()

        if self.term is not None:
            yield from self.ring(0, rows, self.term, self.stage[0], keep)
        yield from self.ring(1, size, held, self.stage[-1], third)
        yield from self.around(2, terms, size)
        part = size // 2
        for k in COLOURS:
            for start in (0, part):
                total = sum(self.a2[k, n * size + start : n * size + start + part, :].astype(F32) for n in range(SIDE)).astype(BF16)
                self.w[row(k, position(k, 0, 0), position(k, 1, 0) * size + start, part), :] = total
                again = total.astype(F32)
                self.ns[k] += jnp.sum((again * again).reshape(-1, 8, LANES), axis=0)
        yield from self.around(1, second, size)
        last = self.around(0, first, rows)
        next(last)
        give(0)
        yield
        next(last)
        give(NEXT, LAST)
        yield
        for _ in last:
            pass
        give(FAR)
        yield
        for copy in given:
            copy.wait_recv()
        stored = self.w.at[pl.ds(0, PER_CORE * rows)]
        for sem in (self.lsem, self.ssem.at[self.ssem.shape[0] - 1]):
            pltpu.make_async_copy(stored, stored, sem).wait()


def _squares(links, ns, nd, nrm, tiles, ssem, rsem):
    sent = []

    def send(ref, other):
        sent.append(_remote(ref, ref, ssem.at[len(sent)], rsem.at[len(sent)], other))
        sent[-1].start()
        return sent[-1]

    totals = [tiles[0, k] + tiles[1, k] for k in COLOURS]
    for dim in (1, 0):
        first, more = {}, {}
        for k in COLOURS:
            slot = ns.at[dim, k, links.position(k, dim, 0)]
            slot[...] = totals[k]
            first[k] = [send(slot, side[ORDERS[k][dim]]) for side in (links.plus, links.minus)]
        yield
        for k in COLOURS:
            for copy in first[k]:
                copy.wait_recv()
            more[k] = send(ns.at[dim, k, links.position(k, dim, LAST)], links.plus[ORDERS[k][dim]])
        yield
        for k in COLOURS:
            more[k].wait_recv()
        totals = [sum(ns[dim, k, n] for n in range(SIDE)) for k in COLOURS]
    nd[links.core] = sum(totals)
    more = send(nd.at[links.core], links.partner)
    yield
    more.wait_recv()
    nrm[...] = nd[0] + nd[1]
    for copy in sent:
        copy.wait_send()


def _tail(x_ref, dy_ref, db_ref, h_ref, q_ref, k_ref, v_ref, o_ref, lse_ref, turns_ref, wo_ref, sum_ref, out_m, out_a, nrm,
          at_s, ot_s, dh_s, do_s, delta_s, kt_s, dq_s, dk_s, dv_s, ga_s, ra_s, *rest):
    refs = iter(rest)
    take = lambda n: [next(refs) for _ in range(n)]
    stage_m, stage_a = [take(3)], [take(3), take(3)]
    a2_m, a1_a, a2_a, w_m, w_a, tiles, ns, nd, lsem = take(9)
    sems = take(6)
    links = _Links()
    links.greet()
    mine, theirs = links.core * PER_CORE, (1 - links.core) * PER_CORE
    tiles[...] = jnp.zeros_like(tiles)

    def attention(k, place, start, n):
        j = SIDE * k + place
        return ga_s[mine + j, start : start + n, :].astype(F32) + ra_s[j, start : start + n, :].astype(F32)

    waves = _Flow(links, 0, None, sum_ref, a2_m, stage_m, w_m, out_m, tiles.at[0], *sems[:2], lsem.at[0]).run()
    attn = _Flow(links, 1, attention, a1_a, a2_a, stage_a, w_a, out_a, tiles.at[1], *sems[2:4], lsem.at[1])

    kt_s[...] = k_ref[...].T
    dk_s[...] = jnp.zeros_like(dk_s)
    dv_s[...] = jnp.zeros_like(dv_s)

    def turned_back(t, rows):
        t = t.astype(BF16).astype(F32)
        cos, sin = _turning(turns_ref, rows)
        return (t * cos + pltpu.roll(t * sin, HALF, 1)).astype(BF16)

    for i in range(TOKENS // STRIP):
        rows = _span(i, STRIP)
        keys = rows.stop
        h, db = h_ref[rows, :].astype(F32), db_ref[rows, :].astype(F32)
        scale = _scale(h)
        by_scale = jnp.sum(db * h, -1, keepdims=True)
        dh = (db * scale - h * (by_scale * scale * scale * scale * (1 / D))).astype(BF16).astype(F32)
        dh = (dy_ref[rows, :].astype(F32) + dh).astype(BF16)
        dh_s[rows, :] = dh
        do = _nt(dh, wo_ref[...]).astype(BF16)
        o = o_ref[rows, :]
        ot_s[:, rows] = o.T
        x = x_ref[rows, :].astype(F32)
        at_s[:, rows] = (x * _scale(x)).astype(BF16).T
        for g in range(HEADS):
            do_s[g, rows, :] = do[:, _lanes(g)]
            both = do[:, _lanes(g)].astype(F32) * o[:, _lanes(g)].astype(F32)
            delta_s[g, :, rows] = jnp.sum(both.T, axis=0, keepdims=True)
        if i == 0:
            links.met()
        next(waves)

        def head(g):
            q, do_g = q_ref[g, rows, :], do_s[g, rows, :]
            s = _nt(k_ref[:keys, :], q)
            own = _hide(s[i * STRIP :, :], 0, 0)
            s = own if i == 0 else jnp.concatenate([s[: i * STRIP, :], own], axis=0)
            p = jnp.exp2(s * (SCALE * LOG2E) - lse_ref[g, :, rows])
            ds = (p * (_nt(v_ref[:keys, :], do_g) - delta_s[g, :, rows])).astype(BF16)
            dv_s[:keys, :] += _nn(p.astype(BF16), do_g)
            dk_s[:keys, :] += _nn(ds, q)
            dq = (_nn(kt_s[:, :keys], ds) * SCALE).T
            dq_s[g, rows, :] = turned_back(dq, rows)

        pl.loop(0, HEADS)(head)
        if keys < TOKENS:
            next(waves)

    every = slice(None)
    dqkv = [dq_s[g] for g in range(HEADS)] + [turned_back(dk_s[...] * SCALE, every), dv_s[...].astype(BF16)]
    dqkv = _nn(at_s[...], jnp.concatenate(dqkv, axis=1)).astype(BF16)
    dwo = _nn(ot_s[...], dh_s[...]).astype(BF16)
    for r in range(8):
        j, rows = r // SIDE * PER_CORE + r % SIDE, _span(r, EIGHTH)
        for t in range(HEADS):
            here = _span(t, EIGHTH)
            ga_s[j, here, :] = dqkv[rows, _lanes(t)]
            ga_s[j + SIDE, here, :] = dwo[rows, _lanes(t)]
            ga_s[j + 2 * SIDE, here, :] = dqkv[rows, _lanes(HEADS + t)] if t < 2 else jnp.zeros((EIGHTH, LANES), BF16)
    a1_a[:, ATTN:, :] = jnp.zeros((3, PADDED[1] - ATTN, LANES), F32)
    other_half = attn.send(ga_s.at[pl.ds(theirs, PER_CORE)], ra_s, links.partner)
    other_half.wait_recv()
    attn.drain()
    attn = attn.run()
    next(attn)
    next(waves)
    for _ in range(6):
        next(attn)
    running = [attn, _squares(links, ns, nd, nrm, tiles, *sems[4:])]
    done = object()
    while running:
        running = [one for one in running if next(one, done) is not done]
    for _ in waves:
        pass


def tail(x, dy, db, h, q, k, v, o, lse, turns, wo, sums):
    vmem = lambda *shape: pltpu.VMEM(shape, BF16)
    wide = lambda *shape: pltpu.VMEM(shape, F32)
    sems = lambda *n: [pltpu.SemaphoreType.DMA((one,)) for one in n]

    def stage(size):
        low = -(-size // (2 * TILE)) * TILE
        return [vmem(3, 3, size, LANES), vmem(3, 2, low, LANES), vmem(3, 2, size, LANES)]

    pieces = [vmem(PER_CORE * rows, LANES) for rows in PADDED]
    (_, m2), (_, b2) = STEPS
    return pl.pallas_call(
        _tail,
        in_specs=[IN_VMEM] * 12,
        out_specs=[ANYWHERE] * 2 + [IN_VMEM],
        out_shape=[jax.ShapeDtypeStruct((PIECES, MLP, LANES), BF16), jax.ShapeDtypeStruct((PIECES, ATTN, LANES), BF16),
                   jax.ShapeDtypeStruct((8, LANES), F32)],
        scratch_shapes=[vmem(D, TOKENS), vmem(D, TOKENS), vmem(TOKENS, D), vmem(HEADS, TOKENS, HEAD), wide(HEADS, 1, TOKENS),
                        vmem(HEAD, TOKENS), vmem(HEADS, TOKENS, HEAD), wide(TOKENS, HEAD), wide(TOKENS, HEAD),
                        vmem(PIECES, ATTN, LANES), vmem(PER_CORE, ATTN, LANES),
                        *stage(m2), *stage(ATTN), *stage(b2),
                        vmem(3, PADDED[0], LANES), wide(3, PADDED[1], LANES), vmem(3, PADDED[1], LANES), *pieces,
                        wide(2, 3, 8, LANES), wide(2, 3, SIDE, 8, LANES), wide(2, 8, LANES), *sems(2, 5, 60, 7, 73, 19, 19)],
        compiler_params=_params(collective_id=0, has_side_effects=True),
        cost_estimate=pl.CostEstimate(flops=8 * 10**9, transcendentals=4 * 10**6, bytes_accessed=40 * 10**6),
        name="tail",
    )(x, dy, db, h, q, k, v, o, lse, turns, wo, sums)


def adamw(w, m, v, g):
    m = 0.9 * m + 0.1 * g
    v = 0.95 * v + 0.05 * g * g
    step = m * lax.rsqrt(v + 1e-8) + 0.1 * w
    return (w - 0.02 * step).astype(BF16), m, v


THIRD = WAVES // 3


def _adam(nrm_ref, gm_ref, ga_ref, *refs):
    total = jnp.sum(jnp.sum(nrm_ref[...], axis=0, keepdims=True), axis=1, keepdims=True)
    factor = jnp.minimum(1.0, 0.5 * lax.rsqrt(total / (3 * D * FF + 2 * D * (D + HEAD)) + 1e-30))
    wq, wk, wv, wo, gate, up, down = (refs[i::7] for i in range(7))

    def step(refs, where, g):
        w, m, v, new_w, new_m, new_v = refs
        new_w[where], new_m[where], new_v[where] = adamw(w[where].astype(F32), m[where], v[where], g.astype(F32) * factor)

    for n in range(THIRD):
        for t in range(3):
            here = _span(3 * n + t, EIGHTH)
            for k, refs in enumerate((gate, up)):
                step(refs, (slice(None), _lanes(3 * n + t)), gm_ref[0, k, 0, here, :])
        for t in range(5):
            here = _span(5 * n + t, DOWN)
            step(down, (n, 0, slice(None), _lanes(t)), gm_ref[0, 2, 0, here, :])

    @pl.when(pl.program_id(1) == 2)
    def _():
        for k, refs in enumerate((wq, wo)):
            for t in range(HEADS):
                step(refs, (slice(None), _lanes(t)), ga_ref[0, k, 0, _span(t, EIGHTH), :])
        for t, refs in enumerate((wk, wv)):
            step(refs, (slice(None), slice(None)), ga_ref[0, 2, 0, _span(t, EIGHTH), :])


def adam(nrm, gm, ga, *wmv):
    small = lambda width: pl.BlockSpec((EIGHTH, width), lambda r, i: (r, 0))
    across = pl.BlockSpec((EIGHTH, THIRD * BLOCK), lambda r, i: (r, i))
    specs = [small(D), small(HEAD), small(HEAD), small(D), across, across, pl.BlockSpec((THIRD, 1, DOWN, D), lambda r, i: (i, r, 0, 0))] * 3
    given = [one.reshape(WAVES, 8, DOWN, D) if one.shape[0] == FF else one for one in wmv]
    pieces = lambda g: g.reshape(2, 3, 4, -1, LANES)
    got = pl.pallas_call(
        _adam,
        grid=(8, 3),
        in_specs=[
            pl.BlockSpec((8, LANES), lambda r, i: (0, 0)),
            pl.BlockSpec((1, 3, 1, THIRD * WAVE, LANES), lambda r, i: (r // 4, 0, r % 4, i, 0)),
            pl.BlockSpec((1, 3, 1, ATTN, LANES), lambda r, i: (r // 4, 0, r % 4, 0, 0)),
            *specs,
        ],
        out_specs=specs,
        out_shape=[jax.ShapeDtypeStruct(one.shape, one.dtype) for one in given],
        compiler_params=_params(dimension_semantics=("arbitrary", "arbitrary")),
        cost_estimate=pl.CostEstimate(flops=10**8, transcendentals=8 * 10**6, bytes_accessed=168 * 10**6),
        name="adam",
    )(nrm, pieces(gm), pieces(ga), *given)
    return [one.reshape(was.shape) for one, was in zip(got, wmv, strict=True)]


def solution(mesh):
    def step(x, dy, *arrays):
        x, dy = x[0], dy[0]
        given = [one[0] for one in arrays]
        wq, wk, wv, wo, gate, up, down = given[:7]
        turns = _turns()
        q, k, v, o, h, b, bt, lse = front(x, turns, wq, wk, wv, wo)
        sums, db = mlp(b, bt, dy, gate, up, down)
        gm, ga, nrm = tail(x, dy, db, h, q, k, v, o, lse, turns, wo, sums)
        return tuple(one[None] for one in adam(nrm, gm, ga, *given))

    states, all_of = P(("rep", "dp"), None, None), P(None, None, None)
    return jax.shard_map(
        step,
        mesh=mesh,
        in_specs=(states, states) + (all_of,) * 21,
        out_specs=(P("rep", None, None),) * 21,
        check_vma=False,
    )
```

```python
import jax
import jax.numpy as jnp
import numpy as np
from jax import lax
from jax.experimental import pallas as pl
from jax.experimental.pallas import tpu as pltpu
from jax.sharding import PartitionSpec as P

BF16, F32 = jnp.bfloat16, jnp.float32
LANES = 128
TOKENS, D, HEADS, FF = 1024, 640, 5, 3456
HEAD, HALF = LANES, LANES // 2
THETA = 10000
HIDDEN = -1e30
SCALE = HEAD**-0.5
LOG2E = 1.4426950408889634
VMEM = 56 * 2**20
STRIP = 256
EIGHTH, DOWN = 80, 48
WAVES, BLOCK = 9, 384
WAVE, ATTN = 240, 400
MLP = WAVES * WAVE
STEPS = ((MLP, 576), (ATTN, 128))
LOW = 128
SIDE = 4
SLOTS = 5
NEXT, FAR, LAST = 1, 2, 3
PADDED = tuple(SIDE * rows for _, rows in STEPS)
STRIDES = (32, 8, 2)
ORDERS = ((0, 1, 2), (1, 2, 0), (2, 0, 1))
COLOURS = range(3)
TILE = 16
PER_CORE, PIECES = 12, 24


def _dot(a, b, ca, cb):
    return lax.dot_general(a, b, (((ca,), (cb,)), ((), ())), preferred_element_type=F32)


def _nn(a, b):
    return _dot(a, b, 1, 0)


def _nt(a, b):
    return _dot(a, b, 1, 1)


def _scale(wide):
    return lax.rsqrt(jnp.mean(wide * wide, -1, keepdims=True) + 1e-6)


def _span(n, size):
    return slice(n * size, n * size + size)


def _lanes(n):
    return _span(n, LANES)


def _turning(turns_ref, rows):
    table = turns_ref[rows, :]
    other = pltpu.roll(table, HALF, 1)
    first = lax.broadcasted_iota(jnp.int32, table.shape, 1) < HALF
    return jnp.where(first, table, other), jnp.where(first, -other, table)


def _hide(s, first_key, first_query):
    key = lax.broadcasted_iota(jnp.int32, s.shape, 0) + first_key
    query = lax.broadcasted_iota(jnp.int32, s.shape, 1) + first_query
    return jnp.where(query >= key, s, HIDDEN)


def _front(x_ref, turns_ref, wq_ref, wk_ref, wv_ref, wo_ref, *rest):
    outs, held, (vt_s, sem) = rest[:8], rest[8:16], rest[16:]
    q_s, k_s, v_s, o_s, h_s, b_s, bt_s, lse_s = held
    copies = []
    wkv = jnp.concatenate([wk_ref[...], wv_ref[...]], axis=1)
    vt_s[HEAD:, :] = jnp.ones((vt_s.shape[0] - HEAD, TOKENS), BF16)
    for i in range(TOKENS // STRIP):
        rows = _span(i, STRIP)
        keys = rows.stop
        x = x_ref[rows, :].astype(F32)
        a = (x * _scale(x)).astype(BF16)
        cos, sin = _turning(turns_ref, rows)

        def turned(t):
            t = t.astype(BF16).astype(F32)
            return (t * cos + pltpu.roll(t, HALF, 1) * sin).astype(BF16)

        q = _nn(a, wq_ref[...])
        for g in range(HEADS):
            q_s[g, rows, :] = turned(q[:, _lanes(g)])
        kv = _nn(a, wkv)
        k_s[rows, :] = turned(kv[:, :HEAD])
        v = kv[:, HEAD:].astype(BF16)
        v_s[rows, :] = v
        vt_s[:HEAD, rows] = v.T
        for g in range(HEADS):
            s = _nt(k_s[:keys, :], q_s[g, rows, :])
            own = _hide(s[i * STRIP :, :], 0, 0)
            s = own if i == 0 else jnp.concatenate([s[: i * STRIP, :], own], axis=0)
            top = jnp.max(s, axis=0, keepdims=True)
            p = jnp.exp2((s - top) * (SCALE * LOG2E)).astype(BF16)
            mix = _nn(vt_s[:, :keys], p)
            total = mix[HEAD : HEAD + 1, :]
            o_s[rows, _lanes(g)] = (mix[:HEAD, :] * (1 / total)).T.astype(BF16)
            lse_s[g, :, rows] = top * (SCALE * LOG2E) + jnp.log2(total)
        h = (x + _nn(o_s[rows, :], wo_ref[...]).astype(BF16).astype(F32)).astype(BF16)
        h_s[rows, :] = h
        h = h.astype(F32)
        b = (h * _scale(h)).astype(BF16)
        b_s[rows, :] = b
        bt_s[:, rows] = b.T
        for src, dst in zip(held, outs, strict=True):
            if src is q_s:
                src, dst = src.at[:, rows, :], dst.at[:, rows, :]
            elif src is bt_s:
                src, dst = src.at[:, rows], dst.at[:, rows]
            elif src is lse_s:
                src, dst = src.at[:, :, rows], dst.at[:, :, rows]
            else:
                src, dst = src.at[rows, :], dst.at[rows, :]
            copies.append(pltpu.make_async_copy(src, dst, sem.at[len(copies)]))
            copies[-1].start()
    for copy in copies:
        copy.wait()


def _params(**more):
    return pltpu.CompilerParams(vmem_limit_bytes=VMEM, **more)


def _turns():
    angle = np.arange(TOKENS)[:, None] * float(THETA) ** (-np.arange(HALF) / HALF)
    return jnp.asarray(np.concatenate([np.cos(angle), np.sin(angle)], 1), F32)


ANYWHERE = pl.BlockSpec(memory_space=pl.ANY)
IN_VMEM = pl.BlockSpec(memory_space=pltpu.VMEM)


def front(x, turns, wq, wk, wv, wo):
    shapes = [((HEADS, TOKENS, HEAD), BF16), ((TOKENS, HEAD), BF16), ((TOKENS, HEAD), BF16), ((TOKENS, D), BF16), ((TOKENS, D), BF16),
              ((TOKENS, D), BF16), ((D, TOKENS), BF16), ((HEADS, 1, TOKENS), F32)]
    return pl.pallas_call(
        _front,
        in_specs=[IN_VMEM] * 6,
        out_specs=[ANYWHERE] * 8,
        out_shape=[jax.ShapeDtypeStruct(*one) for one in shapes],
        scratch_shapes=[pltpu.VMEM(*one) for one in shapes] + [pltpu.VMEM((HEAD + 8, TOKENS), BF16), pltpu.SemaphoreType.DMA((32,))],
        compiler_params=_params(),
        cost_estimate=pl.CostEstimate(flops=5 * 10**9, transcendentals=4 * 10**6, bytes_accessed=15 * 10**6),
        name="front",
    )(x, turns, wq, wk, wv, wo)


class _Links:
    def __init__(self):
        me = lax.axis_index("dp")
        self.at = [lax.rem(lax.div(me, stride), SIDE) for stride in STRIDES]
        self.core = lax.rem(me, 2)
        self.partner = me + 1 - 2 * self.core

        def along(d, q):
            return me + STRIDES[d] * (lax.rem(self.at[d] + q, SIDE) - self.at[d])

        self.plus, self.minus = ([along(d, q) for d in range(3)] for q in (NEXT, LAST))

    def greet(self):
        for other in (*self.plus, *self.minus, self.partner):
            pl.semaphore_signal(pltpu.get_barrier_semaphore(), inc=1, device_id={"dp": other}, device_id_type=pl.DeviceIdType.MESH)

    def met(self):
        pl.semaphore_wait(pltpu.get_barrier_semaphore(), 7)

    def position(self, k, dim, q):
        return lax.rem(self.at[ORDERS[k][dim]] + q, SIDE)


def _remote(src, dst, send_sem, recv_sem, other):
    return pltpu.make_async_remote_copy(src_ref=src, dst_ref=dst, send_sem=send_sem, recv_sem=recv_sem, device_id={"dp": other},
                                        device_id_type=pl.DeviceIdType.MESH)


def _mlp(b_ref, bt_ref, dy_ref, wg_ref, wu_ref, wd_ref, sum_ref, db_ref, acc, g_s, r_s, lo_s, hi_s, two_s, ssem, rsem):
    f = pl.program_id(0)
    links = _Links()
    mine, theirs = links.core * PER_CORE, (1 - links.core) * PER_CORE
    low, high = slice(0, LOW), slice(LOW, WAVE)

    def pair(u):
        return _remote(g_s.at[u, pl.ds(theirs, PER_CORE)], r_s.at[u], ssem.at[u % SLOTS], rsem.at[u % SLOTS, 0], links.partner)

    def message(u, k, n):
        d, back = ORDERS[k][0], n % 2
        rows = (low, high)[n in (1, 2, 5)]
        src = g_s.at[u, mine + SIDE * k + links.position(k, 0, FAR if n < 2 else (NEXT, LAST)[back]), rows]
        dst = (lo_s, hi_s)[n].at[u, k] if n < 2 else two_s.at[u, k, back, rows]
        return _remote(src, dst, ssem.at[u % SLOTS], rsem.at[u % SLOTS, 6 * k + n + 1], (links.minus if back else links.plus)[d])

    def both(u, k, q, rows):
        j = SIDE * k + links.position(k, 0, q)
        return g_s[u, mine + j, rows, :].astype(F32) + r_s[u, j, rows, :].astype(F32)

    def put(u, k, q, rows, total):
        g_s[u, mine + SIDE * k + links.position(k, 0, q), rows, :] = total.astype(BF16)

    def stage(lag):
        u = f - lag
        return lambda run: pl.when((u >= 0) & (u < WAVES))(lambda: run(u))

    @pl.when(f == 0)
    def _():
        links.greet()

    @pl.when(f == 1)
    def _():
        links.met()

    @stage(1)
    def _(u):
        pair(u).start()

    @stage(2)
    def _(u):
        pair(u).wait_recv()
        for k in COLOURS:
            for n, (q, rows) in enumerate(((FAR, low), (FAR, high), (NEXT, high), (LAST, low))):
                put(u, k, q, rows, both(u, k, q, rows))
                message(u, k, n).start()

    @stage(3)
    def _(u):
        for k in COLOURS:
            message(u, k, 0).wait_recv()
            put(u, k, NEXT, low, both(u, k, NEXT, low) + lo_s[u, k].astype(F32))
            message(u, k, 4).start()
            message(u, k, 1).wait_recv()
            put(u, k, LAST, high, both(u, k, LAST, high) + hi_s[u, k].astype(F32))
            message(u, k, 5).start()

    @stage(4)
    def _(u):
        for k in COLOURS:
            for n in range(2, 6):
                message(u, k, n).wait_recv()
            for rows in (low, high):
                here = pl.ds(pl.multiple_of(u * WAVE + rows.start, TILE), rows.stop - rows.start)
                sum_ref[k, here, :] = both(u, k, 0, rows) + two_s[u, k, 0, rows, :].astype(F32) + two_s[u, k, 1, rows, :].astype(F32)
        sent = g_s.at[u, pl.ds(0, 21)]
        pltpu.make_async_copy(sent, sent, ssem.at[u % SLOTS]).wait()

    @pl.when(f < WAVES)
    def _():
        wgu = jnp.concatenate([wg_ref[...], wu_ref[...]], axis=1)
        gu = _nn(b_ref[...], wgu)
        gate, up = gu[:, :BLOCK], gu[:, BLOCK:]
        dact = _nt(dy_ref[...], wd_ref[...]).astype(BF16).astype(F32)
        s = 0.5 * jnp.tanh(0.5 * gate) + 0.5
        silu = gate * s
        act = (silu * up).astype(BF16)
        dgu = jnp.concatenate([(dact * up * (s + silu * (1 - s))).astype(BF16), (dact * silu).astype(BF16)], axis=1)
        dw = _nn(bt_ref[...], dgu).astype(BF16)
        dwd = _dot(act, dy_ref[...], 0, 0).astype(BF16)
        for r in range(8):
            j = r // SIDE * PER_CORE + r % SIDE
            for n in range(6):
                g_s[f, j + n // 3 * SIDE, _span(n % 3, EIGHTH), :] = dw[_span(r, EIGHTH), _lanes(n)]
            for t in range(HEADS):
                g_s[f, j + 2 * SIDE, _span(t, DOWN), :] = dwd[_span(r, DOWN), _lanes(t)]
        acc[...] = jnp.where(f > 0, acc[...], 0.0) + _nt(dgu, wgu)

    @pl.when(f == WAVES - 1)
    def _():
        db_ref[...] = acc[...].astype(BF16)

    @pl.when(f == WAVES + 3)
    def _():
        sum_ref[:, MLP:, :] = jnp.zeros((3, PADDED[0] - MLP, LANES), F32)


def mlp(b, bt, dy, wg, wu, wd):
    vmem = lambda *shape: pltpu.VMEM((*shape, LANES), BF16)
    whole = lambda *shape: pl.BlockSpec(shape, lambda f: (0,) * len(shape), pipeline_mode=pl.Buffered(1))
    across = pl.BlockSpec((D, BLOCK), lambda f: (0, jnp.minimum(f, WAVES - 1)))
    down = pl.BlockSpec((BLOCK, D), lambda f: (jnp.minimum(f, WAVES - 1), 0))
    return pl.pallas_call(
        _mlp,
        grid=(WAVES + 4,),
        in_specs=[whole(TOKENS, D), whole(D, TOKENS), whole(TOKENS, D), across, across, down],
        out_specs=[whole(3, PADDED[0], LANES), whole(TOKENS, D)],
        out_shape=[jax.ShapeDtypeStruct((3, PADDED[0], LANES), F32), jax.ShapeDtypeStruct((TOKENS, D), BF16)],
        scratch_shapes=[pltpu.VMEM((TOKENS, D), F32), vmem(WAVES, PIECES, WAVE), vmem(WAVES, PER_CORE, WAVE), vmem(WAVES, 3, LOW),
                        vmem(WAVES, 3, WAVE - LOW), vmem(WAVES, 3, 2, WAVE), pltpu.SemaphoreType.DMA((SLOTS,)), pltpu.SemaphoreType.DMA((SLOTS, 19))],
        compiler_params=_params(dimension_semantics=("arbitrary",), collective_id=1, has_side_effects=True),
        cost_estimate=pl.CostEstimate(flops=16 * TOKENS * D * FF, transcendentals=TOKENS * FF, bytes_accessed=40 * 2**20),
        name="mlp",
    )(b, bt, dy, wg, wu, wd)


class _Flow:
    def __init__(self, links, part, term, a1, a2, stage, w, out, ns, ssem, rsem, lsem):
        self.links, self.part, self.term, self.a1, self.a2, self.stage, self.w, self.out, self.ns = links, part, term, a1, a2, stage, w, out, ns
        self.ssem, self.rsem, self.lsem, self.received, self.groups = ssem, rsem, lsem, 0, 0
        self.rows = 0

    def send(self, src, dst, other, given=False):
        copy = _remote(src, dst, self.ssem.at[self.ssem.shape[0] - 1 if given else self.groups], self.rsem.at[self.received], other)
        copy.start()
        self.received += 1
        self.rows += 0 if given else src.size // LANES
        return copy

    def drain(self):
        sent = self.w.at[pl.ds(0, self.rows)]
        pltpu.make_async_copy(sent, sent, self.ssem.at[self.groups]).wait()
        self.groups += 1
        self.rows = 0

    def sides(self, k, dim):
        return (side[ORDERS[k][dim]] for side in (self.links.plus, self.links.minus))

    def ring(self, dim, size, term, stage, store):
        staged, first, second = stage
        low = first.shape[2]
        high = size - low
        position = self.links.position
        relays, rest = {}, {}

        def fill(k, slot, q, start, n, more=None):
            total = term(k, position(k, dim, q), start, n)
            if more is not None:
                total += first[k, more, :n, :].astype(F32)
            staged[k, slot, start : start + n, :] = total.astype(BF16)

        for k in COLOURS:
            plus, minus = self.sides(k, dim)
            fill(k, 0, FAR, 0, low)
            fill(k, 0, FAR, low, high)
            relays[k] = [self.send(staged.at[k, 0, :low], first.at[k, 0], plus), self.send(staged.at[k, 0, low:], first.at[k, 1, :high], minus)]
            fill(k, 1, NEXT, low, high)
            fill(k, 2, LAST, 0, low)
        yield
        for k in COLOURS:
            plus, minus = self.sides(k, dim)
            relays[k][0].wait_recv()
            fill(k, 1, NEXT, 0, low, 0)
            rest[k] = [self.send(staged.at[k, 1], second.at[k, 0], plus)]
            relays[k][1].wait_recv()
            fill(k, 2, LAST, low, high, 1)
            rest[k] += [self.send(staged.at[k, 2], second.at[k, 1], minus)]
        yield
        for k in COLOURS:
            for copy in rest[k]:
                copy.wait_recv()
            for start in range(0, size, low):
                here = slice(start, min(start + low, size))
                total = term(k, position(k, dim, 0), start, here.stop - start)
                store(k, start, total + second[k, 0, here, :].astype(F32) + second[k, 1, here, :].astype(F32))
        self.drain()

    def around(self, dim, block, size):
        low = -(-size // (2 * TILE)) * TILE
        first, second = {}, {}
        for k in COLOURS:
            first[k] = [self.send(block(k, 0, 0, size), block(k, 0, 0, size), side) for side in self.sides(k, dim)]
        yield
        for k in COLOURS:
            plus, minus = self.sides(k, dim)
            first[k][0].wait_recv()
            second[k] = [self.send(block(k, LAST, 0, low), block(k, LAST, 0, low), plus)]
            first[k][1].wait_recv()
            second[k] += [self.send(block(k, NEXT, low, size - low), block(k, NEXT, low, size - low), minus)]
        yield
        for k in COLOURS:
            for copy in second[k]:
                copy.wait_recv()
        self.drain()

    def run(self):
        position = self.links.position
        rows, size = STEPS[self.part]
        whole = PADDED[self.part]
        mine = self.links.core * PER_CORE
        given = []

        def keep(k, i, total):
            self.a1[k, i : i + total.shape[0], :] = total

        def held(k, place, start, n):
            return self.a1[k, pl.ds(pl.multiple_of(place * size + start, TILE), n), :]

        def third(k, i, total):
            self.a2[k, pl.ds(pl.multiple_of(position(k, 2, 0) * size + i, TILE), total.shape[0]), :] = total.astype(BF16)

        def terms(k, q, start, n):
            return self.a2.at[k, pl.ds(pl.multiple_of(position(k, 2, q) * size + start, TILE), n)]

        def row(k, piece, start, n):
            return pl.ds(pl.multiple_of((SIDE * k + piece) * whole + start, TILE), n)

        def second(k, q, start, n):
            return self.w.at[row(k, position(k, 0, 0), position(k, 1, q) * size + start, n)]

        def first(k, q, start, n):
            return self.w.at[row(k, position(k, 0, q), start, n)]

        def give(*distances):
            for q in distances:
                for k in COLOURS:
                    src, dst = first(k, q, 0, rows), self.out.at[mine + SIDE * k + position(k, 0, q)]
                    given.append(self.send(src, dst, self.links.partner, True))
                    pltpu.make_async_copy(src, dst, self.lsem).start()

        if self.term is not None:
            yield from self.ring(0, rows, self.term, self.stage[0], keep)
        yield from self.ring(1, size, held, self.stage[-1], third)
        yield from self.around(2, terms, size)
        part = size // 2
        for k in COLOURS:
            for start in (0, part):
                total = sum(self.a2[k, n * size + start : n * size + start + part, :].astype(F32) for n in range(SIDE)).astype(BF16)
                self.w[row(k, position(k, 0, 0), position(k, 1, 0) * size + start, part), :] = total
                again = total.astype(F32)
                self.ns[k] += jnp.sum((again * again).reshape(-1, 8, LANES), axis=0)
        yield from self.around(1, second, size)
        last = self.around(0, first, rows)
        next(last)
        give(0)
        yield
        next(last)
        give(NEXT, LAST)
        yield
        for _ in last:
            pass
        give(FAR)
        yield
        for copy in given:
            copy.wait_recv()
        stored = self.w.at[pl.ds(0, PER_CORE * rows)]
        for sem in (self.lsem, self.ssem.at[self.ssem.shape[0] - 1]):
            pltpu.make_async_copy(stored, stored, sem).wait()


def _squares(links, ns, nd, nrm, tiles, ssem, rsem):
    sent = []

    def send(ref, other):
        sent.append(_remote(ref, ref, ssem.at[len(sent)], rsem.at[len(sent)], other))
        sent[-1].start()
        return sent[-1]

    totals = [tiles[0, k] + tiles[1, k] for k in COLOURS]
    for dim in (1, 0):
        first, more = {}, {}
        for k in COLOURS:
            slot = ns.at[dim, k, links.position(k, dim, 0)]
            slot[...] = totals[k]
            first[k] = [send(slot, side[ORDERS[k][dim]]) for side in (links.plus, links.minus)]
        yield
        for k in COLOURS:
            for copy in first[k]:
                copy.wait_recv()
            more[k] = send(ns.at[dim, k, links.position(k, dim, LAST)], links.plus[ORDERS[k][dim]])
        yield
        for k in COLOURS:
            more[k].wait_recv()
        totals = [sum(ns[dim, k, n] for n in range(SIDE)) for k in COLOURS]
    nd[links.core] = sum(totals)
    more = send(nd.at[links.core], links.partner)
    yield
    more.wait_recv()
    nrm[...] = nd[0] + nd[1]
    for copy in sent:
        copy.wait_send()


def _tail(x_ref, dy_ref, db_ref, h_ref, q_ref, k_ref, v_ref, o_ref, lse_ref, turns_ref, wo_ref, sum_ref, out_m, out_a, nrm,
          at_s, ot_s, dh_s, do_s, delta_s, kt_s, dq_s, dk_s, dv_s, ga_s, ra_s, *rest):
    refs = iter(rest)
    take = lambda n: [next(refs) for _ in range(n)]
    stage_m, stage_a = [take(3)], [take(3), take(3)]
    a2_m, a1_a, a2_a, w_m, w_a, tiles, ns, nd, lsem = take(9)
    sems = take(6)
    links = _Links()
    links.greet()
    mine, theirs = links.core * PER_CORE, (1 - links.core) * PER_CORE
    tiles[...] = jnp.zeros_like(tiles)

    def attention(k, place, start, n):
        j = SIDE * k + place
        return ga_s[mine + j, start : start + n, :].astype(F32) + ra_s[j, start : start + n, :].astype(F32)

    waves = _Flow(links, 0, None, sum_ref, a2_m, stage_m, w_m, out_m, tiles.at[0], *sems[:2], lsem.at[0]).run()
    attn = _Flow(links, 1, attention, a1_a, a2_a, stage_a, w_a, out_a, tiles.at[1], *sems[2:4], lsem.at[1])

    kt_s[...] = k_ref[...].T
    dk_s[...] = jnp.zeros_like(dk_s)
    dv_s[...] = jnp.zeros_like(dv_s)

    def turned_back(t, rows):
        t = t.astype(BF16).astype(F32)
        cos, sin = _turning(turns_ref, rows)
        return (t * cos + pltpu.roll(t * sin, HALF, 1)).astype(BF16)

    for i in range(TOKENS // STRIP):
        rows = _span(i, STRIP)
        keys = rows.stop
        h, db = h_ref[rows, :].astype(F32), db_ref[rows, :].astype(F32)
        scale = _scale(h)
        by_scale = jnp.sum(db * h, -1, keepdims=True)
        dh = (db * scale - h * (by_scale * scale * scale * scale * (1 / D))).astype(BF16).astype(F32)
        dh = (dy_ref[rows, :].astype(F32) + dh).astype(BF16)
        dh_s[rows, :] = dh
        do = _nt(dh, wo_ref[...]).astype(BF16)
        o = o_ref[rows, :]
        ot_s[:, rows] = o.T
        x = x_ref[rows, :].astype(F32)
        at_s[:, rows] = (x * _scale(x)).astype(BF16).T
        for g in range(HEADS):
            do_s[g, rows, :] = do[:, _lanes(g)]
            both = do[:, _lanes(g)].astype(F32) * o[:, _lanes(g)].astype(F32)
            delta_s[g, :, rows] = jnp.sum(both.T, axis=0, keepdims=True)
        if i == 0:
            links.met()
        next(waves)

        def head(g):
            q, do_g = q_ref[g, rows, :], do_s[g, rows, :]
            s = _nt(k_ref[:keys, :], q)
            own = _hide(s[i * STRIP :, :], 0, 0)
            s = own if i == 0 else jnp.concatenate([s[: i * STRIP, :], own], axis=0)
            p = jnp.exp2(s * (SCALE * LOG2E) - lse_ref[g, :, rows])
            ds = (p * (_nt(v_ref[:keys, :], do_g) - delta_s[g, :, rows])).astype(BF16)
            dv_s[:keys, :] += _nn(p.astype(BF16), do_g)
            dk_s[:keys, :] += _nn(ds, q)
            dq = (_nn(kt_s[:, :keys], ds) * SCALE).T
            dq_s[g, rows, :] = turned_back(dq, rows)

        pl.loop(0, HEADS)(head)
        if keys < TOKENS:
            next(waves)

    every = slice(None)
    dqkv = [dq_s[g] for g in range(HEADS)] + [turned_back(dk_s[...] * SCALE, every), dv_s[...].astype(BF16)]
    dqkv = _nn(at_s[...], jnp.concatenate(dqkv, axis=1)).astype(BF16)
    dwo = _nn(ot_s[...], dh_s[...]).astype(BF16)
    for r in range(8):
        j, rows = r // SIDE * PER_CORE + r % SIDE, _span(r, EIGHTH)
        for t in range(HEADS):
            here = _span(t, EIGHTH)
            ga_s[j, here, :] = dqkv[rows, _lanes(t)]
            ga_s[j + SIDE, here, :] = dwo[rows, _lanes(t)]
            ga_s[j + 2 * SIDE, here, :] = dqkv[rows, _lanes(HEADS + t)] if t < 2 else jnp.zeros((EIGHTH, LANES), BF16)
    a1_a[:, ATTN:, :] = jnp.zeros((3, PADDED[1] - ATTN, LANES), F32)
    other_half = attn.send(ga_s.at[pl.ds(theirs, PER_CORE)], ra_s, links.partner)
    next(waves)
    other_half.wait_recv()
    attn.drain()
    attn = attn.run()
    next(attn)
    for _ in range(6):
        next(attn)
    running = [_squares(links, ns, nd, nrm, tiles, *sems[4:]), attn, waves]
    done = object()
    while running:
        running = [one for one in running if next(one, done) is not done]


def tail(x, dy, db, h, q, k, v, o, lse, turns, wo, sums):
    vmem = lambda *shape: pltpu.VMEM(shape, BF16)
    wide = lambda *shape: pltpu.VMEM(shape, F32)
    sems = lambda *n: [pltpu.SemaphoreType.DMA((one,)) for one in n]

    def stage(size):
        low = -(-size // (2 * TILE)) * TILE
        return [vmem(3, 3, size, LANES), vmem(3, 2, low, LANES), vmem(3, 2, size, LANES)]

    pieces = [vmem(PER_CORE * rows, LANES) for rows in PADDED]
    (_, m2), (_, b2) = STEPS
    return pl.pallas_call(
        _tail,
        in_specs=[IN_VMEM] * 12,
        out_specs=[ANYWHERE] * 2 + [IN_VMEM],
        out_shape=[jax.ShapeDtypeStruct((PIECES, MLP, LANES), BF16), jax.ShapeDtypeStruct((PIECES, ATTN, LANES), BF16),
                   jax.ShapeDtypeStruct((8, LANES), F32)],
        scratch_shapes=[vmem(D, TOKENS), vmem(D, TOKENS), vmem(TOKENS, D), vmem(HEADS, TOKENS, HEAD), wide(HEADS, 1, TOKENS),
                        vmem(HEAD, TOKENS), vmem(HEADS, TOKENS, HEAD), wide(TOKENS, HEAD), wide(TOKENS, HEAD),
                        vmem(PIECES, ATTN, LANES), vmem(PER_CORE, ATTN, LANES),
                        *stage(m2), *stage(ATTN), *stage(b2),
                        vmem(3, PADDED[0], LANES), wide(3, PADDED[1], LANES), vmem(3, PADDED[1], LANES), *pieces,
                        wide(2, 3, 8, LANES), wide(2, 3, SIDE, 8, LANES), wide(2, 8, LANES), *sems(2, 5, 60, 7, 73, 19, 19)],
        compiler_params=_params(collective_id=0, has_side_effects=True),
        cost_estimate=pl.CostEstimate(flops=8 * 10**9, transcendentals=4 * 10**6, bytes_accessed=40 * 10**6),
        name="tail",
    )(x, dy, db, h, q, k, v, o, lse, turns, wo, sums)


def adamw(w, m, v, g):
    m = 0.9 * m + 0.1 * g
    v = 0.95 * v + 0.05 * g * g
    step = m * lax.rsqrt(v + 1e-8) + 0.1 * w
    return (w - 0.02 * step).astype(BF16), m, v


THIRD = WAVES


def _adam(nrm_ref, gm_ref, ga_ref, *refs):
    total = jnp.sum(jnp.sum(nrm_ref[...], axis=0, keepdims=True), axis=1, keepdims=True)
    factor = jnp.minimum(1.0, 0.5 * lax.rsqrt(total / (3 * D * FF + 2 * D * (D + HEAD)) + 1e-30))
    wq, wk, wv, wo, gate, up, down = (refs[i::7] for i in range(7))

    def step(refs, where, g):
        w, m, v, new_w, new_m, new_v = refs
        new_w[where], new_m[where], new_v[where] = adamw(w[where].astype(F32), m[where], v[where], g.astype(F32) * factor)

    for n in range(THIRD):
        for t in range(3):
            here = _span(3 * n + t, EIGHTH)
            for k, refs in enumerate((gate, up)):
                step(refs, (slice(None), _lanes(3 * n + t)), gm_ref[0, k, 0, here, :])
        for t in range(5):
            here = _span(5 * n + t, DOWN)
            step(down, (n, 0, slice(None), _lanes(t)), gm_ref[0, 2, 0, here, :])

    @pl.when(pl.program_id(1) == WAVES // THIRD - 1)
    def _():
        for k, refs in enumerate((wq, wo)):
            for t in range(HEADS):
                step(refs, (slice(None), _lanes(t)), ga_ref[0, k, 0, _span(t, EIGHTH), :])
        for t, refs in enumerate((wk, wv)):
            step(refs, (slice(None), slice(None)), ga_ref[0, 2, 0, _span(t, EIGHTH), :])


def adam(nrm, gm, ga, *wmv):
    small = lambda width: pl.BlockSpec((EIGHTH, width), lambda r, i: (r, 0))
    across = pl.BlockSpec((EIGHTH, THIRD * BLOCK), lambda r, i: (r, i))
    specs = [small(D), small(HEAD), small(HEAD), small(D), across, across, pl.BlockSpec((THIRD, 1, DOWN, D), lambda r, i: (i, r, 0, 0))] * 3
    given = [one.reshape(WAVES, 8, DOWN, D) if one.shape[0] == FF else one for one in wmv]
    pieces = lambda g: g.reshape(2, 3, 4, -1, LANES)
    got = pl.pallas_call(
        _adam,
        grid=(8, WAVES // THIRD),
        in_specs=[
            pl.BlockSpec((8, LANES), lambda r, i: (0, 0)),
            pl.BlockSpec((1, 3, 1, THIRD * WAVE, LANES), lambda r, i: (r // 4, 0, r % 4, i, 0)),
            pl.BlockSpec((1, 3, 1, ATTN, LANES), lambda r, i: (r // 4, 0, r % 4, 0, 0)),
            *specs,
        ],
        out_specs=specs,
        out_shape=[jax.ShapeDtypeStruct(one.shape, one.dtype) for one in given],
        compiler_params=_params(dimension_semantics=("arbitrary", "arbitrary")),
        cost_estimate=pl.CostEstimate(flops=10**8, transcendentals=8 * 10**6, bytes_accessed=168 * 10**6),
        name="adam",
    )(nrm, pieces(gm), pieces(ga), *given)
    return [one.reshape(was.shape) for one, was in zip(got, wmv, strict=True)]


def solution(mesh):
    def step(x, dy, *arrays):
        x, dy = x[0], dy[0]
        given = [one[0] for one in arrays]
        wq, wk, wv, wo, gate, up, down = given[:7]
        turns = _turns()
        q, k, v, o, h, b, bt, lse = front(x, turns, wq, wk, wv, wo)
        sums, db = mlp(b, bt, dy, gate, up, down)
        gm, ga, nrm = tail(x, dy, db, h, q, k, v, o, lse, turns, wo, sums)
        return tuple(one[None] for one in adam(nrm, gm, ga, *given))

    states, all_of = P(("rep", "dp"), None, None), P(None, None, None)
    return jax.shard_map(
        step,
        mesh=mesh,
        in_specs=(states, states) + (all_of,) * 21,
        out_specs=(P("rep", None, None),) * 21,
        check_vma=False,
    )
```

```python
import jax
import jax.numpy as jnp
import numpy as np
from jax import lax
from jax.experimental import pallas as pl
from jax.experimental.pallas import tpu as pltpu
from jax.sharding import PartitionSpec as P

BF16, F32 = jnp.bfloat16, jnp.float32
LANES = 128
TOKENS, D, HEADS, FF = 1024, 640, 5, 3456
HEAD, HALF = LANES, LANES // 2
THETA = 10000
HIDDEN = -1e30
SCALE = HEAD**-0.5
LOG2E = 1.4426950408889634
VMEM = 60 * 2**20
STRIP = 256
EIGHTH, DOWN = 80, 48
WAVES, BLOCK = 9, 384
WAVE, ATTN = 240, 400
MLP = WAVES * WAVE
STEPS = ((MLP, 576), (ATTN, 128))
LOW = 128
SIDE = 4
SLOTS = 6
NEXT, FAR, LAST = 1, 2, 3
PADDED = tuple(SIDE * rows for _, rows in STEPS)
STRIDES = (32, 8, 2)
ORDERS = ((0, 1, 2), (1, 2, 0), (2, 0, 1))
COLOURS = range(3)
TILE = 16
PER_CORE, PIECES = 12, 24


def _dot(a, b, ca, cb):
    return lax.dot_general(a, b, (((ca,), (cb,)), ((), ())), preferred_element_type=F32)


def _nn(a, b):
    return _dot(a, b, 1, 0)


def _nt(a, b):
    return _dot(a, b, 1, 1)


def _scale(wide):
    return lax.rsqrt(jnp.mean(wide * wide, -1, keepdims=True) + 1e-6)


def _span(n, size):
    return slice(n * size, n * size + size)


def _lanes(n):
    return _span(n, LANES)


def _turning(turns_ref, rows):
    table = turns_ref[rows, :]
    other = pltpu.roll(table, HALF, 1)
    first = lax.broadcasted_iota(jnp.int32, table.shape, 1) < HALF
    return jnp.where(first, table, other), jnp.where(first, -other, table)


def _hide(s, first_key, first_query):
    key = lax.broadcasted_iota(jnp.int32, s.shape, 0) + first_key
    query = lax.broadcasted_iota(jnp.int32, s.shape, 1) + first_query
    return jnp.where(query >= key, s, HIDDEN)


def _front(x_ref, turns_ref, wq_ref, wk_ref, wv_ref, wo_ref, *rest):
    outs, held, (vt_s, sem) = rest[:8], rest[8:16], rest[16:]
    q_s, k_s, v_s, o_s, h_s, b_s, bt_s, lse_s = held
    copies = []
    wkv = jnp.concatenate([wk_ref[...], wv_ref[...]], axis=1)
    vt_s[HEAD:, :] = jnp.ones((vt_s.shape[0] - HEAD, TOKENS), BF16)
    for i in range(TOKENS // STRIP):
        rows = _span(i, STRIP)
        keys = rows.stop
        x = x_ref[rows, :].astype(F32)
        a = (x * _scale(x)).astype(BF16)
        cos, sin = _turning(turns_ref, rows)

        def turned(t):
            t = t.astype(BF16).astype(F32)
            return (t * cos + pltpu.roll(t, HALF, 1) * sin).astype(BF16)

        q = _nn(a, wq_ref[...])
        for g in range(HEADS):
            q_s[g, rows, :] = turned(q[:, _lanes(g)])
        kv = _nn(a, wkv)
        k_s[rows, :] = turned(kv[:, :HEAD])
        v = kv[:, HEAD:].astype(BF16)
        v_s[rows, :] = v
        vt_s[:HEAD, rows] = v.T
        for g in range(HEADS):
            s = _nt(k_s[:keys, :], q_s[g, rows, :])
            own = _hide(s[i * STRIP :, :], 0, 0)
            s = own if i == 0 else jnp.concatenate([s[: i * STRIP, :], own], axis=0)
            top = jnp.max(s, axis=0, keepdims=True)
            p = jnp.exp2((s - top) * (SCALE * LOG2E)).astype(BF16)
            mix = _nn(vt_s[:, :keys], p)
            total = mix[HEAD : HEAD + 1, :]
            o_s[rows, _lanes(g)] = (mix[:HEAD, :] * (1 / total)).T.astype(BF16)
            lse_s[g, :, rows] = top * (SCALE * LOG2E) + jnp.log2(total)
        h = (x + _nn(o_s[rows, :], wo_ref[...]).astype(BF16).astype(F32)).astype(BF16)
        h_s[rows, :] = h
        h = h.astype(F32)
        b = (h * _scale(h)).astype(BF16)
        b_s[rows, :] = b
        bt_s[:, rows] = b.T
        for src, dst in zip(held, outs, strict=True):
            if src is q_s:
                src, dst = src.at[:, rows, :], dst.at[:, rows, :]
            elif src is bt_s:
                src, dst = src.at[:, rows], dst.at[:, rows]
            elif src is lse_s:
                src, dst = src.at[:, :, rows], dst.at[:, :, rows]
            else:
                src, dst = src.at[rows, :], dst.at[rows, :]
            copies.append(pltpu.make_async_copy(src, dst, sem.at[len(copies)]))
            copies[-1].start()
    for copy in copies:
        copy.wait()


def _params(**more):
    return pltpu.CompilerParams(vmem_limit_bytes=VMEM, **more)


def _turns():
    angle = np.arange(TOKENS)[:, None] * float(THETA) ** (-np.arange(HALF) / HALF)
    return jnp.asarray(np.concatenate([np.cos(angle), np.sin(angle)], 1), F32)


ANYWHERE = pl.BlockSpec(memory_space=pl.ANY)
IN_VMEM = pl.BlockSpec(memory_space=pltpu.VMEM)


def front(x, turns, wq, wk, wv, wo):
    shapes = [((HEADS, TOKENS, HEAD), BF16), ((TOKENS, HEAD), BF16), ((TOKENS, HEAD), BF16), ((TOKENS, D), BF16), ((TOKENS, D), BF16),
              ((TOKENS, D), BF16), ((D, TOKENS), BF16), ((HEADS, 1, TOKENS), F32)]
    return pl.pallas_call(
        _front,
        in_specs=[IN_VMEM] * 6,
        out_specs=[ANYWHERE] * 8,
        out_shape=[jax.ShapeDtypeStruct(*one) for one in shapes],
        scratch_shapes=[pltpu.VMEM(*one) for one in shapes] + [pltpu.VMEM((HEAD + 8, TOKENS), BF16), pltpu.SemaphoreType.DMA((32,))],
        compiler_params=_params(),
        cost_estimate=pl.CostEstimate(flops=5 * 10**9, transcendentals=4 * 10**6, bytes_accessed=15 * 10**6),
        name="front",
    )(x, turns, wq, wk, wv, wo)


class _Links:
    def __init__(self):
        me = lax.axis_index("dp")
        self.at = [lax.rem(lax.div(me, stride), SIDE) for stride in STRIDES]
        self.core = lax.rem(me, 2)
        self.partner = me + 1 - 2 * self.core

        def along(d, q):
            return me + STRIDES[d] * (lax.rem(self.at[d] + q, SIDE) - self.at[d])

        self.plus, self.minus = ([along(d, q) for d in range(3)] for q in (NEXT, LAST))

    def greet(self):
        for other in (*self.plus, *self.minus, self.partner):
            pl.semaphore_signal(pltpu.get_barrier_semaphore(), inc=1, device_id={"dp": other}, device_id_type=pl.DeviceIdType.MESH)

    def met(self):
        pl.semaphore_wait(pltpu.get_barrier_semaphore(), 7)

    def position(self, k, dim, q):
        return lax.rem(self.at[ORDERS[k][dim]] + q, SIDE)


def _remote(src, dst, send_sem, recv_sem, other):
    return pltpu.make_async_remote_copy(src_ref=src, dst_ref=dst, send_sem=send_sem, recv_sem=recv_sem, device_id={"dp": other},
                                        device_id_type=pl.DeviceIdType.MESH)


def _mlp(b_ref, bt_ref, dy_ref, wg_ref, wu_ref, wd_ref, sum_ref, db_ref, acc, dgu_s, g_s, r_s, lo_s, hi_s, two_s, ssem, rsem):
    f = pl.program_id(0)
    late = jnp.maximum(f - WAVES, 0)
    time = f - late + late // 3
    links = _Links()
    mine, theirs = links.core * PER_CORE, (1 - links.core) * PER_CORE
    low, high = slice(0, LOW), slice(LOW, WAVE)

    def pair(u):
        return _remote(g_s.at[u % SLOTS, pl.ds(theirs, PER_CORE)], r_s.at[u % SLOTS], ssem.at[u % SLOTS], rsem.at[u % SLOTS, 0], links.partner)

    def message(u, k, n):
        d, back = ORDERS[k][0], n % 2
        rows = (low, high)[n in (1, 2, 5)]
        src = g_s.at[u % SLOTS, mine + SIDE * k + links.position(k, 0, FAR if n < 2 else (NEXT, LAST)[back]), rows]
        dst = (lo_s, hi_s)[n].at[u % SLOTS, k] if n < 2 else two_s.at[u % SLOTS, k, back, rows]
        return _remote(src, dst, ssem.at[u % SLOTS], rsem.at[u % SLOTS, 6 * k + n + 1], (links.minus if back else links.plus)[d])

    def both(u, k, q, rows):
        j = SIDE * k + links.position(k, 0, q)
        return g_s[u % SLOTS, mine + j, rows, :].astype(F32) + r_s[u % SLOTS, j, rows, :].astype(F32)

    def put(u, k, q, rows, total):
        g_s[u % SLOTS, mine + SIDE * k + links.position(k, 0, q), rows, :] = total.astype(BF16)

    def stage(lag):
        u = time - lag
        return lambda run: pl.when((u >= 0) & (u < WAVES) & (late % 3 == 0))(lambda: run(u))

    @pl.when(f == 0)
    def _():
        links.greet()

    @pl.when(f == 1)
    def _():
        links.met()

    @stage(1)
    def _(u):
        pair(u).start()

    @stage(2)
    def _(u):
        pair(u).wait_recv()
        for k in COLOURS:
            for n, (q, rows) in enumerate(((FAR, low), (FAR, high), (NEXT, high), (LAST, low))):
                put(u, k, q, rows, both(u, k, q, rows))
                message(u, k, n).start()

    @stage(3)
    def _(u):
        for k in COLOURS:
            message(u, k, 0).wait_recv()
            put(u, k, NEXT, low, both(u, k, NEXT, low) + lo_s[u % SLOTS, k].astype(F32))
            message(u, k, 4).start()
            message(u, k, 1).wait_recv()
            put(u, k, LAST, high, both(u, k, LAST, high) + hi_s[u % SLOTS, k].astype(F32))
            message(u, k, 5).start()

    @stage(4)
    def _(u):
        for k in COLOURS:
            for n in range(2, 6):
                message(u, k, n).wait_recv()
            for rows in (low, high):
                here = pl.ds(pl.multiple_of(u * WAVE + rows.start, TILE), rows.stop - rows.start)
                sum_ref[k, here, :] = both(u, k, 0, rows) + two_s[u % SLOTS, k, 0, rows, :].astype(F32) + two_s[u % SLOTS, k, 1, rows, :].astype(F32)
        sent = g_s.at[u % SLOTS, pl.ds(0, 21)]
        pltpu.make_async_copy(sent, sent, ssem.at[u % SLOTS]).wait()

    @pl.when(f < WAVES)
    def _():
        wgu = jnp.concatenate([wg_ref[...], wu_ref[...]], axis=1)
        gu = _nn(b_ref[...], wgu)
        gate, up = gu[:, :BLOCK], gu[:, BLOCK:]
        dact = _nt(dy_ref[...], wd_ref[...]).astype(BF16).astype(F32)
        s = 0.5 * jnp.tanh(0.5 * gate) + 0.5
        silu = gate * s
        act = (silu * up).astype(BF16)
        dgu = jnp.concatenate([(dact * up * (s + silu * (1 - s))).astype(BF16), (dact * silu).astype(BF16)], axis=1)
        dw = _nn(bt_ref[...], dgu).astype(BF16)
        dwd = _dot(act, dy_ref[...], 0, 0).astype(BF16)
        for r in range(8):
            j = r // SIDE * PER_CORE + r % SIDE
            for n in range(6):
                g_s[f % SLOTS, j + n // 3 * SIDE, _span(n % 3, EIGHTH), :] = dw[_span(r, EIGHTH), _lanes(n)]
            for t in range(HEADS):
                g_s[f % SLOTS, j + 2 * SIDE, _span(t, DOWN), :] = dwd[_span(r, DOWN), _lanes(t)]
        dgu_s[f] = dgu

    @pl.when((f >= WAVES) & (f < 2 * WAVES))
    def _():
        more = _nt(dgu_s[late], jnp.concatenate([wg_ref[...], wu_ref[...]], axis=1))
        acc[...] = jnp.where(late > 0, acc[...], 0.0) + more

    @pl.when(f == 2 * WAVES)
    def _():
        db_ref[...] = acc[...].astype(BF16)
        sum_ref[:, MLP:, :] = jnp.zeros((3, PADDED[0] - MLP, LANES), F32)


def mlp(b, bt, dy, wg, wu, wd):
    vmem = lambda *shape: pltpu.VMEM((*shape, LANES), BF16)
    whole = lambda *shape: pl.BlockSpec(shape, lambda f: (0,) * len(shape), pipeline_mode=pl.Buffered(1))
    across = pl.BlockSpec((D, BLOCK), lambda f: (0, jnp.where(f < WAVES, f, jnp.minimum(f - WAVES, WAVES - 1))))
    down = pl.BlockSpec((BLOCK, D), lambda f: (jnp.minimum(f, WAVES - 1), 0))
    return pl.pallas_call(
        _mlp,
        grid=(2 * WAVES + 1,),
        in_specs=[whole(TOKENS, D), whole(D, TOKENS), whole(TOKENS, D), across, across, down],
        out_specs=[whole(3, PADDED[0], LANES), whole(TOKENS, D)],
        out_shape=[jax.ShapeDtypeStruct((3, PADDED[0], LANES), F32), jax.ShapeDtypeStruct((TOKENS, D), BF16)],
        scratch_shapes=[pltpu.VMEM((TOKENS, D), F32), pltpu.VMEM((WAVES, TOKENS, 2 * BLOCK), BF16), vmem(SLOTS, PIECES, WAVE),
                        vmem(SLOTS, PER_CORE, WAVE), vmem(SLOTS, 3, LOW), vmem(SLOTS, 3, WAVE - LOW), vmem(SLOTS, 3, 2, WAVE),
                        pltpu.SemaphoreType.DMA((SLOTS,)), pltpu.SemaphoreType.DMA((SLOTS, 19))],
        compiler_params=_params(dimension_semantics=("arbitrary",), collective_id=1, has_side_effects=True),
        cost_estimate=pl.CostEstimate(flops=16 * TOKENS * D * FF, transcendentals=TOKENS * FF, bytes_accessed=40 * 2**20),
        name="mlp",
    )(b, bt, dy, wg, wu, wd)


class _Flow:
    def __init__(self, links, part, term, a1, a2, stage, w, out, ns, ssem, rsem, lsem):
        self.links, self.part, self.term, self.a1, self.a2, self.stage, self.w, self.out, self.ns = links, part, term, a1, a2, stage, w, out, ns
        self.ssem, self.rsem, self.lsem, self.received, self.groups = ssem, rsem, lsem, 0, 0
        self.rows = 0

    def send(self, src, dst, other, given=False):
        copy = _remote(src, dst, self.ssem.at[self.ssem.shape[0] - 1 if given else self.groups], self.rsem.at[self.received], other)
        copy.start()
        self.received += 1
        self.rows += 0 if given else src.size // LANES
        return copy

    def drain(self):
        sent = self.w.at[pl.ds(0, self.rows)]
        pltpu.make_async_copy(sent, sent, self.ssem.at[self.groups]).wait()
        self.groups += 1
        self.rows = 0

    def sides(self, k, dim):
        return (side[ORDERS[k][dim]] for side in (self.links.plus, self.links.minus))

    def ring(self, dim, size, term, stage, store):
        staged, first, second = stage
        low = first.shape[2]
        high = size - low
        position = self.links.position
        relays, rest = {}, {}

        def fill(k, slot, q, start, n, more=None):
            total = term(k, position(k, dim, q), start, n)
            if more is not None:
                total += first[k, more, :n, :].astype(F32)
            staged[k, slot, start : start + n, :] = total.astype(BF16)

        for k in COLOURS:
            plus, minus = self.sides(k, dim)
            fill(k, 0, FAR, 0, low)
            fill(k, 0, FAR, low, high)
            relays[k] = [self.send(staged.at[k, 0, :low], first.at[k, 0], plus), self.send(staged.at[k, 0, low:], first.at[k, 1, :high], minus)]
            fill(k, 1, NEXT, low, high)
            fill(k, 2, LAST, 0, low)
        yield
        for k in COLOURS:
            plus, minus = self.sides(k, dim)
            relays[k][0].wait_recv()
            fill(k, 1, NEXT, 0, low, 0)
            rest[k] = [self.send(staged.at[k, 1], second.at[k, 0], plus)]
            relays[k][1].wait_recv()
            fill(k, 2, LAST, low, high, 1)
            rest[k] += [self.send(staged.at[k, 2], second.at[k, 1], minus)]
        yield
        for k in COLOURS:
            for copy in rest[k]:
                copy.wait_recv()
            for start in range(0, size, low):
                here = slice(start, min(start + low, size))
                total = term(k, position(k, dim, 0), start, here.stop - start)
                store(k, start, total + second[k, 0, here, :].astype(F32) + second[k, 1, here, :].astype(F32))
        self.drain()

    def around(self, dim, block, size):
        low = -(-size // (2 * TILE)) * TILE
        first, second = {}, {}
        for k in COLOURS:
            first[k] = [self.send(block(k, 0, 0, size), block(k, 0, 0, size), side) for side in self.sides(k, dim)]
        yield
        for k in COLOURS:
            plus, minus = self.sides(k, dim)
            first[k][0].wait_recv()
            second[k] = [self.send(block(k, LAST, 0, low), block(k, LAST, 0, low), plus)]
            first[k][1].wait_recv()
            second[k] += [self.send(block(k, NEXT, low, size - low), block(k, NEXT, low, size - low), minus)]
        yield
        for k in COLOURS:
            for copy in second[k]:
                copy.wait_recv()
        self.drain()

    def run(self):
        position = self.links.position
        rows, size = STEPS[self.part]
        whole = PADDED[self.part]
        mine = self.links.core * PER_CORE
        given = []

        def keep(k, i, total):
            self.a1[k, i : i + total.shape[0], :] = total

        def held(k, place, start, n):
            return self.a1[k, pl.ds(pl.multiple_of(place * size + start, TILE), n), :]

        def third(k, i, total):
            self.a2[k, pl.ds(pl.multiple_of(position(k, 2, 0) * size + i, TILE), total.shape[0]), :] = total.astype(BF16)

        def terms(k, q, start, n):
            return self.a2.at[k, pl.ds(pl.multiple_of(position(k, 2, q) * size + start, TILE), n)]

        def row(k, piece, start, n):
            return pl.ds(pl.multiple_of((SIDE * k + piece) * whole + start, TILE), n)

        def second(k, q, start, n):
            return self.w.at[row(k, position(k, 0, 0), position(k, 1, q) * size + start, n)]

        def first(k, q, start, n):
            return self.w.at[row(k, position(k, 0, q), start, n)]

        def give(*distances):
            for q in distances:
                for k in COLOURS:
                    src, dst = first(k, q, 0, rows), self.out.at[mine + SIDE * k + position(k, 0, q)]
                    given.append(self.send(src, dst, self.links.partner, True))
                    pltpu.make_async_copy(src, dst, self.lsem).start()

        if self.term is not None:
            yield from self.ring(0, rows, self.term, self.stage[0], keep)
        yield from self.ring(1, size, held, self.stage[-1], third)
        yield from self.around(2, terms, size)
        part = size // 2
        for k in COLOURS:
            for start in (0, part):
                total = sum(self.a2[k, n * size + start : n * size + start + part, :].astype(F32) for n in range(SIDE)).astype(BF16)
                self.w[row(k, position(k, 0, 0), position(k, 1, 0) * size + start, part), :] = total
                again = total.astype(F32)
                self.ns[k] += jnp.sum((again * again).reshape(-1, 8, LANES), axis=0)
        yield from self.around(1, second, size)
        last = self.around(0, first, rows)
        next(last)
        give(0)
        yield
        next(last)
        give(NEXT, LAST)
        yield
        for _ in last:
            pass
        give(FAR)
        yield
        for copy in given:
            copy.wait_recv()
        stored = self.w.at[pl.ds(0, PER_CORE * rows)]
        for sem in (self.lsem, self.ssem.at[self.ssem.shape[0] - 1]):
            pltpu.make_async_copy(stored, stored, sem).wait()


def _squares(links, ns, nd, nrm, tiles, ssem, rsem):
    sent = []

    def send(ref, other):
        sent.append(_remote(ref, ref, ssem.at[len(sent)], rsem.at[len(sent)], other))
        sent[-1].start()
        return sent[-1]

    totals = [tiles[0, k] + tiles[1, k] for k in COLOURS]
    for dim in (1, 0):
        first, more = {}, {}
        for k in COLOURS:
            slot = ns.at[dim, k, links.position(k, dim, 0)]
            slot[...] = totals[k]
            first[k] = [send(slot, side[ORDERS[k][dim]]) for side in (links.plus, links.minus)]
        yield
        for k in COLOURS:
            for copy in first[k]:
                copy.wait_recv()
            more[k] = send(ns.at[dim, k, links.position(k, dim, LAST)], links.plus[ORDERS[k][dim]])
        yield
        for k in COLOURS:
            more[k].wait_recv()
        totals = [sum(ns[dim, k, n] for n in range(SIDE)) for k in COLOURS]
    nd[links.core] = sum(totals)
    more = send(nd.at[links.core], links.partner)
    yield
    more.wait_recv()
    nrm[...] = nd[0] + nd[1]
    for copy in sent:
        copy.wait_send()


def _tail(x_ref, dy_ref, db_ref, h_ref, q_ref, k_ref, v_ref, o_ref, lse_ref, turns_ref, wo_ref, sum_ref, out_m, out_a, nrm,
          at_s, ot_s, dh_s, do_s, delta_s, kt_s, dq_s, dk_s, dv_s, ga_s, ra_s, *rest):
    refs = iter(rest)
    take = lambda n: [next(refs) for _ in range(n)]
    stage_m, stage_a = [take(3)], [take(3), take(3)]
    a2_m, a1_a, a2_a, w_m, w_a, tiles, ns, nd, lsem = take(9)
    sems = take(6)
    links = _Links()
    links.greet()
    mine, theirs = links.core * PER_CORE, (1 - links.core) * PER_CORE
    tiles[...] = jnp.zeros_like(tiles)

    def attention(k, place, start, n):
        j = SIDE * k + place
        return ga_s[mine + j, start : start + n, :].astype(F32) + ra_s[j, start : start + n, :].astype(F32)

    waves = _Flow(links, 0, None, sum_ref, a2_m, stage_m, w_m, out_m, tiles.at[0], *sems[:2], lsem.at[0]).run()
    attn = _Flow(links, 1, attention, a1_a, a2_a, stage_a, w_a, out_a, tiles.at[1], *sems[2:4], lsem.at[1])

    kt_s[...] = k_ref[...].T
    dk_s[...] = jnp.zeros_like(dk_s)
    dv_s[...] = jnp.zeros_like(dv_s)

    def turned_back(t, rows):
        t = t.astype(BF16).astype(F32)
        cos, sin = _turning(turns_ref, rows)
        return (t * cos + pltpu.roll(t * sin, HALF, 1)).astype(BF16)

    for i in range(TOKENS // STRIP):
        rows = _span(i, STRIP)
        keys = rows.stop
        h, db = h_ref[rows, :].astype(F32), db_ref[rows, :].astype(F32)
        scale = _scale(h)
        by_scale = jnp.sum(db * h, -1, keepdims=True)
        dh = (db * scale - h * (by_scale * scale * scale * scale * (1 / D))).astype(BF16).astype(F32)
        dh = (dy_ref[rows, :].astype(F32) + dh).astype(BF16)
        dh_s[rows, :] = dh
        do = _nt(dh, wo_ref[...]).astype(BF16)
        o = o_ref[rows, :]
        ot_s[:, rows] = o.T
        x = x_ref[rows, :].astype(F32)
        at_s[:, rows] = (x * _scale(x)).astype(BF16).T
        for g in range(HEADS):
            do_s[g, rows, :] = do[:, _lanes(g)]
            both = do[:, _lanes(g)].astype(F32) * o[:, _lanes(g)].astype(F32)
            delta_s[g, :, rows] = jnp.sum(both.T, axis=0, keepdims=True)
        if i == 0:
            links.met()
        next(waves)

        def head(g):
            q, do_g = q_ref[g, rows, :], do_s[g, rows, :]
            s = _nt(k_ref[:keys, :], q)
            own = _hide(s[i * STRIP :, :], 0, 0)
            s = own if i == 0 else jnp.concatenate([s[: i * STRIP, :], own], axis=0)
            p = jnp.exp2(s * (SCALE * LOG2E) - lse_ref[g, :, rows])
            ds = (p * (_nt(v_ref[:keys, :], do_g) - delta_s[g, :, rows])).astype(BF16)
            dv_s[:keys, :] += _nn(p.astype(BF16), do_g)
            dk_s[:keys, :] += _nn(ds, q)
            dq = (_nn(kt_s[:, :keys], ds) * SCALE).T
            dq_s[g, rows, :] = turned_back(dq, rows)

        pl.loop(0, HEADS)(head)
        if keys < TOKENS:
            next(waves)

    every = slice(None)
    dqkv = [dq_s[g] for g in range(HEADS)] + [turned_back(dk_s[...] * SCALE, every), dv_s[...].astype(BF16)]
    dqkv = _nn(at_s[...], jnp.concatenate(dqkv, axis=1)).astype(BF16)
    dwo = _nn(ot_s[...], dh_s[...]).astype(BF16)
    for r in range(8):
        j, rows = r // SIDE * PER_CORE + r % SIDE, _span(r, EIGHTH)
        for t in range(HEADS):
            here = _span(t, EIGHTH)
            ga_s[j, here, :] = dqkv[rows, _lanes(t)]
            ga_s[j + SIDE, here, :] = dwo[rows, _lanes(t)]
            ga_s[j + 2 * SIDE, here, :] = dqkv[rows, _lanes(HEADS + t)] if t < 2 else jnp.zeros((EIGHTH, LANES), BF16)
    a1_a[:, ATTN:, :] = jnp.zeros((3, PADDED[1] - ATTN, LANES), F32)
    other_half = attn.send(ga_s.at[pl.ds(theirs, PER_CORE)], ra_s, links.partner)
    next(waves)
    other_half.wait_recv()
    attn.drain()
    attn = attn.run()
    next(attn)
    for _ in range(6):
        next(attn)
    running = [_squares(links, ns, nd, nrm, tiles, *sems[4:]), attn, waves]
    done = object()
    while running:
        running = [one for one in running if next(one, done) is not done]


def tail(x, dy, db, h, q, k, v, o, lse, turns, wo, sums):
    vmem = lambda *shape: pltpu.VMEM(shape, BF16)
    wide = lambda *shape: pltpu.VMEM(shape, F32)
    sems = lambda *n: [pltpu.SemaphoreType.DMA((one,)) for one in n]

    def stage(size):
        low = -(-size // (2 * TILE)) * TILE
        return [vmem(3, 3, size, LANES), vmem(3, 2, low, LANES), vmem(3, 2, size, LANES)]

    pieces = [vmem(PER_CORE * rows, LANES) for rows in PADDED]
    (_, m2), (_, b2) = STEPS
    return pl.pallas_call(
        _tail,
        in_specs=[IN_VMEM] * 12,
        out_specs=[ANYWHERE] * 2 + [IN_VMEM],
        out_shape=[jax.ShapeDtypeStruct((PIECES, MLP, LANES), BF16), jax.ShapeDtypeStruct((PIECES, ATTN, LANES), BF16),
                   jax.ShapeDtypeStruct((8, LANES), F32)],
        scratch_shapes=[vmem(D, TOKENS), vmem(D, TOKENS), vmem(TOKENS, D), vmem(HEADS, TOKENS, HEAD), wide(HEADS, 1, TOKENS),
                        vmem(HEAD, TOKENS), vmem(HEADS, TOKENS, HEAD), wide(TOKENS, HEAD), wide(TOKENS, HEAD),
                        vmem(PIECES, ATTN, LANES), vmem(PER_CORE, ATTN, LANES),
                        *stage(m2), *stage(ATTN), *stage(b2),
                        vmem(3, PADDED[0], LANES), wide(3, PADDED[1], LANES), vmem(3, PADDED[1], LANES), *pieces,
                        wide(2, 3, 8, LANES), wide(2, 3, SIDE, 8, LANES), wide(2, 8, LANES), *sems(2, 5, 60, 7, 73, 19, 19)],
        compiler_params=_params(collective_id=0, has_side_effects=True),
        cost_estimate=pl.CostEstimate(flops=8 * 10**9, transcendentals=4 * 10**6, bytes_accessed=40 * 10**6),
        name="tail",
    )(x, dy, db, h, q, k, v, o, lse, turns, wo, sums)


def adamw(w, m, v, g):
    m = 0.9 * m + 0.1 * g
    v = 0.95 * v + 0.05 * g * g
    step = m * lax.rsqrt(v + 1e-8) + 0.1 * w
    return (w - 0.02 * step).astype(BF16), m, v


THIRD = WAVES


def _adam(nrm_ref, gm_ref, ga_ref, *refs):
    total = jnp.sum(jnp.sum(nrm_ref[...], axis=0, keepdims=True), axis=1, keepdims=True)
    factor = jnp.minimum(1.0, 0.5 * lax.rsqrt(total / (3 * D * FF + 2 * D * (D + HEAD)) + 1e-30))
    wq, wk, wv, wo, gate, up, down = (refs[i::7] for i in range(7))

    def step(refs, where, g):
        w, m, v, new_w, new_m, new_v = refs
        new_w[where], new_m[where], new_v[where] = adamw(w[where].astype(F32), m[where], v[where], g.astype(F32) * factor)

    for n in range(THIRD):
        for t in range(3):
            here = _span(3 * n + t, EIGHTH)
            for k, refs in enumerate((gate, up)):
                step(refs, (slice(None), _lanes(3 * n + t)), gm_ref[0, k, 0, here, :])
        for t in range(5):
            here = _span(5 * n + t, DOWN)
            step(down, (n, 0, slice(None), _lanes(t)), gm_ref[0, 2, 0, here, :])

    @pl.when(pl.program_id(1) == WAVES // THIRD - 1)
    def _():
        for k, refs in enumerate((wq, wo)):
            for t in range(HEADS):
                step(refs, (slice(None), _lanes(t)), ga_ref[0, k, 0, _span(t, EIGHTH), :])
        for t, refs in enumerate((wk, wv)):
            step(refs, (slice(None), slice(None)), ga_ref[0, 2, 0, _span(t, EIGHTH), :])


def adam(nrm, gm, ga, *wmv):
    small = lambda width: pl.BlockSpec((EIGHTH, width), lambda r, i: (r, 0))
    across = pl.BlockSpec((EIGHTH, THIRD * BLOCK), lambda r, i: (r, i))
    specs = [small(D), small(HEAD), small(HEAD), small(D), across, across, pl.BlockSpec((THIRD, 1, DOWN, D), lambda r, i: (i, r, 0, 0))] * 3
    given = [one.reshape(WAVES, 8, DOWN, D) if one.shape[0] == FF else one for one in wmv]
    pieces = lambda g: g.reshape(2, 3, 4, -1, LANES)
    got = pl.pallas_call(
        _adam,
        grid=(8, WAVES // THIRD),
        in_specs=[
            pl.BlockSpec((8, LANES), lambda r, i: (0, 0)),
            pl.BlockSpec((1, 3, 1, THIRD * WAVE, LANES), lambda r, i: (r // 4, 0, r % 4, i, 0)),
            pl.BlockSpec((1, 3, 1, ATTN, LANES), lambda r, i: (r // 4, 0, r % 4, 0, 0)),
            *specs,
        ],
        out_specs=specs,
        out_shape=[jax.ShapeDtypeStruct(one.shape, one.dtype) for one in given],
        compiler_params=_params(dimension_semantics=("arbitrary", "arbitrary")),
        cost_estimate=pl.CostEstimate(flops=10**8, transcendentals=8 * 10**6, bytes_accessed=168 * 10**6),
        name="adam",
    )(nrm, pieces(gm), pieces(ga), *given)
    return [one.reshape(was.shape) for one, was in zip(got, wmv, strict=True)]


def solution(mesh):
    def step(x, dy, *arrays):
        x, dy = x[0], dy[0]
        given = [one[0] for one in arrays]
        wq, wk, wv, wo, gate, up, down = given[:7]
        turns = _turns()
        q, k, v, o, h, b, bt, lse = front(x, turns, wq, wk, wv, wo)
        sums, db = mlp(b, bt, dy, gate, up, down)
        gm, ga, nrm = tail(x, dy, db, h, q, k, v, o, lse, turns, wo, sums)
        return tuple(one[None] for one in adam(nrm, gm, ga, *given))

    states, all_of = P(("rep", "dp"), None, None), P(None, None, None)
    return jax.shard_map(
        step,
        mesh=mesh,
        in_specs=(states, states) + (all_of,) * 21,
        out_specs=(P("rep", None, None),) * 21,
        check_vma=False,
    )
```
